32 devices in a mesh: space: 16 (over z, y, x), rep: 2 (over core).
Axes of the slice: x: 2, y: 2, z: 4, core: 2. Of those that a mesh axis runs over, the one named last changes fastest.
Arguments:
- halo_rows: bfloat16 [4, 2048, 256], P(None, 'space', 'rep'), may hold values from -6 to 6
- unmatched: int32 [4, 2048], P(None, 'space'), may hold values 0 or 1
- owner_id: int32 [4, 2048, 1], P(None, 'space'), may hold values from 0 to 15; in each aligned block of 128 rows (0 to 127, 128 to 255, ..., all dimensions but the last counted through in order) at most 16 rows name the same one
- cand_index: int32 [4, 2048, 16], P(None, 'space'), may hold values from 0 to 511
- lengths: int32 [4, 2048], P(None, 'space'), may hold values from 1 to 16
- choice_index: int32 [4, 2048], P(None, 'space'), may hold values from 0 to 15, as said below
- desc_rows: bfloat16 [4, 8192, 256], P(None, 'space', 'rep'), may hold values from -6 to 6
Outputs:
- phantom: bfloat16 [4, 2048, 256], P(None, 'space', 'rep')
- best_merit: bfloat16 [4, 2048], P(None, 'space')
The draws below stay inside these ranges and needn't reach their ends.
Inputs may be any that keep to these rules, and one draw needn't show every extreme that they name: `owner_id`: in each aligned block of 128 halos (one region in one snapshot) no owner is named by more than 16 halos, a bound that some block reaches. `choice_index`: less than the halo's length.
All inputs are finite; a program needn't handle non-finite values. No bound on the sum of `unmatched` on one device may be relied on, other than what follows from the above.
Results may differ from the reference program's by a relative error of at most 0.001.
Values may be sent and summed in bfloat16 or wider, within the bound.
No kernel may reach another device: no remote copies, remote signals or barrier semaphores. Data moves between devices by JAX's collectives and lax.ppermute only.
A program may use at most 64 MiB of HBM per device.

```python
import math
import jax
import jax.numpy as jnp
import numpy as np
from jax import lax

WIDTH = 256
SNAPS = 4
K = 16
HALO_DEV = 128
CAND_DEV = 512
CAP = 16
HALOS = 2048
CANDS = 8192
N_SPACE = 16


def draw_pair(key):
    base_key = jax.random.fold_in(key, 71)
    first_key, second_key = jax.random.split(base_key)
    span_draw = jax.random.randint(first_key, (SNAPS, HALOS), 1, K + 1)
    pick_draw = jax.random.randint(second_key, (SNAPS, HALOS), 0, 1048576) % span_draw
    return (span_draw, pick_draw)


def draw_lengths(key, part):
    return draw_pair(key)[0].astype(jnp.int32)


def draw_choice_index(key, part):
    return draw_pair(key)[1].astype(jnp.int32)


def place_ends(values, rng, smallest, top_value):
    shape = values.shape
    index_at = [jax.random.randint(jax.random.fold_in(rng, axis), (), 0, shape[axis]) for axis in range(len(shape))]
    values = values.at[tuple(index_at)].set(smallest)
    longest = shape.index(max(shape))
    index_at[longest] = (index_at[longest] + 1) % shape[longest]
    return values.at[tuple(index_at)].set(top_value)


def shard_levels(stream_key, extent, shards, low, largest):
    level, own = 1.0, jax.random.fold_in(stream_key, 6)
    for position, parts in shards:
        draws = jnp.exp(jax.random.uniform(jax.random.fold_in(own, position), (parts,), jnp.float32, low / len(shards), largest / len(shards)))
        level = level * jnp.repeat(draws, extent[position] // parts).reshape([-1 if axis == position else 1 for axis in range(len(extent))])
    return level


def routed_block(own_key, own, number, rows, count, top, limit, skew):
    order = jax.random.permutation(own_key, count)
    packed, common = shares(count, rows * top, limit, skew, True), shares(count, rows * top, limit, skew, False)
    places = jnp.arange(count)

    def named(tallies, offset_by):
        used = int((tallies > 0).sum())
        fixed = max(1, used // 4)
        passed = fixed + (places - fixed + offset_by * (used - fixed)) % max(1, count - fixed)
        return jnp.zeros((count,), jnp.int32).at[order[jnp.where(places < fixed, places, passed)]].set(jnp.asarray(tallies, jnp.int32))

    tallies = jnp.where(number % 4 == 0, named(packed, number // 4), named(common, number - number // 4 - 1))
    mixed = jax.random.permutation(jax.random.fold_in(own, 3), count)
    giver, receiver = mixed[0:count // 2 * 2:2], mixed[1:count // 2 * 2:2]
    room = jnp.minimum(tallies[giver] - 1, limit - tallies[receiver]) // 2
    room = jnp.where((giver == order[0]) | (receiver == order[0]) | (tallies[receiver] == 0), 0, jnp.maximum(room, 0))
    passed = jax.random.randint(jax.random.fold_in(own, 4), (count // 2,), 0, 1 << 20) % (room + 1)
    tallies = tallies.at[giver].add(-passed).at[receiver].add(passed)
    items = jnp.searchsorted(jnp.cumsum(tallies), jnp.arange(rows * top), side="right").astype(jnp.int32)
    grid = items.reshape(top, rows).T
    grid = grid[jax.random.permutation(jax.random.fold_in(own, 1), rows)]
    offset_by = jax.random.randint(jax.random.fold_in(own, 2), (rows, 1), 0, top)
    return jnp.take_along_axis(grid, (jnp.arange(top)[None, :] + offset_by) % top, axis=1)


def shares(amount, total, limit, slope, full):
    portions = [(1 << 20) // math.isqrt(rank ** slope) + 1 for rank in range(1, amount + 1)]
    largest = limit if full else min(limit, max(-(-total // amount), total * portions[0] // sum(portions)))
    least = 1 if total - largest >= amount - 1 else 0
    counts, rest = [largest] + [least] * (amount - 1), total - largest - least * (amount - 1)
    while rest > 0:
        movable = [i for i in range(1, amount) if counts[i] < largest] or [i for i in range(1, amount) if counts[i] < limit]
        pool, budget = sum([portions[i] for i in movable]), rest
        for i in movable:
            extra = min(limit - counts[i], max(1, budget * portions[i] // pool), rest)
            counts[i] = counts[i] + extra
            rest = rest - extra
    return np.array(counts)


def noise(own_key, dims, deviation, bound, shards=(), kind=jnp.bfloat16):
    entries = jax.random.normal(own_key, dims, jnp.float32) * deviation
    if len(shards) > 0:
        entries = shard_levels(own_key, dims, shards, -0.22, 0.18) * entries
    return jnp.clip(entries, min=-bound, max=bound).astype(kind)


def setup_inputs(seed: int = 0) -> dict:
    splits = jax.random.split(jax.random.key(seed), 8)
    halo_rows = noise(splits[0], (SNAPS, HALOS, WIDTH), 1.0, 6.0, ((1, 16), (2, 2)))
    unmatched = place_ends((jax.random.randint(splits[1], (SNAPS, HALOS), 0, 3) < 2).astype(jnp.int32), jax.random.fold_in(splits[1], 1), 0, 1)
    owner_id_keys = jax.random.split(jax.random.fold_in(splits[2], 1), SNAPS * HALOS // HALO_DEV)
    owner_id_turns = jax.random.permutation(jax.random.fold_in(splits[2], 3), SNAPS * HALOS // HALO_DEV)
    owner_id = jax.vmap(lambda own, number: routed_block(jax.random.fold_in(splits[2], 2), own, number, HALO_DEV, N_SPACE, 1, CAP, 2))(owner_id_keys, owner_id_turns).reshape((SNAPS, HALOS, 1))
    cand_index = place_ends(jax.random.randint(splits[3], (SNAPS, HALOS, K), 0, CAND_DEV), jax.random.fold_in(splits[3], 1), 0, CAND_DEV - 1).astype(jnp.int32)
    lengths = draw_lengths(jax.random.fold_in(splits[7], 71), 0)
    choice_index = draw_choice_index(jax.random.fold_in(splits[7], 71), 0)
    desc_rows = noise(splits[6], (SNAPS, CANDS, WIDTH), 1.0, 6.0, ((1, 16), (2, 2)))
    return dict(halo_rows=halo_rows, unmatched=unmatched, owner_id=owner_id, cand_index=cand_index, lengths=lengths, choice_index=choice_index, desc_rows=desc_rows)


def reference(halo_rows, unmatched, owner_id, cand_index, lengths, choice_index, desc_rows):
    phantom_list = []
    best_list = []
    lane_ids = jnp.arange(K, dtype=jnp.int32)
    block_size = math.gcd(HALOS, 4096)
    for snapshot in range(SNAPS):
        rows_here = halo_rows[snapshot]
        desc_table = desc_rows[snapshot]
        glob = (owner_id[snapshot, :, 0][:, None] * CAND_DEV + cand_index[snapshot]).astype(jnp.int32)

        def score_block(pieces):
            rows_block, glob_block = pieces
            picked = desc_table[glob_block].astype(jnp.float32)
            return jnp.einsum('rkw,rw->rk', picked, rows_block.astype(jnp.float32))
        merit_full = lax.map(score_block, (rows_here.reshape(-1, block_size, WIDTH), glob.reshape(-1, block_size, K)))
        merit_full = merit_full.reshape(HALOS, K) / math.sqrt(WIDTH)
        live_halo = unmatched[snapshot] == 1
        used = lane_ids[None, :] < lengths[snapshot][:, None]
        live_entry = used & live_halo[:, None]
        quality = 1.0 + jax.nn.softplus(merit_full)
        claims = jnp.zeros((CANDS,), jnp.float32).at[glob.reshape(-1)].max(jnp.where(live_entry, quality, jnp.zeros_like(quality)).reshape(-1))
        pick_pos = choice_index[snapshot][:, None].astype(jnp.int32)
        chosen = jnp.take_along_axis(glob, pick_pos, 1)[:, 0]
        chosen_quality = jnp.take_along_axis(quality, pick_pos, 1)[:, 0]
        share_weight = chosen_quality / (chosen_quality + claims[chosen])
        blended = ((1.0 - share_weight)[:, None] * rows_here.astype(jnp.float32) + share_weight[:, None] * desc_table[chosen].astype(jnp.float32)).astype(jnp.bfloat16)
        phantom_list.append(jnp.where(live_halo[:, None], blended, rows_here))
        top_merit = lax.optimization_barrier(jnp.max(jnp.where(used, merit_full, jnp.full_like(merit_full, -1e+30)), axis=1))
        best_list.append(jnp.where(live_halo, top_merit, jnp.zeros_like(top_merit)).astype(jnp.bfloat16))
    return (jnp.stack(phantom_list), jnp.stack(best_list))
```

```python
import math

import jax
import jax.numpy as jnp
from jax import lax
from jax.experimental import pallas as pl
from jax.experimental.pallas import tpu as pltpu
from jax.sharding import PartitionSpec as P

LANES = 128
SUB = 8
NEG = -3.0e38


def iota(shape, axis):
    return lax.broadcasted_iota(jnp.int32, shape, axis)


def onehot(mask):
    return jnp.where(mask, 1.0, 0.0).astype(jnp.bfloat16)


def dot(a, b, ca, cb):
    return lax.dot_general(a, b, (((ca,), (cb,)), ((), ())), preferred_element_type=jnp.float32)


class Plan:
    def __init__(self, peers, groups, snaps, halos, width, cands, listed):
        self.peers, self.groups, self.snaps = peers, groups, snaps
        self.halos, self.width, self.cands, self.listed = halos, width, cands, listed
        self.per = snaps // groups
        self.slots = 2 * halos // peers
        self.total = peers * self.slots
        self.data = self.per * self.slots
        self.fit = LANES // listed
        self.send = -(-(self.data + -(-self.data // self.fit)) // SUB) * SUB
        self.back = -(-(self.data + 1) // SUB) * SUB
        self.half = cands // 2
        self.aligned = self.slots % SUB == 0
        assert snaps % groups == 0 and groups == 2
        assert width == LANES and halos <= LANES and cands <= 512
        assert LANES % listed == 0 and self.data <= LANES


def route_kernel(plan, owner_ref, live_ref, cand_ref, span_ref, pick_ref, rows_ref, out_ref, target_ref):
    n, h, k = plan.peers, plan.halos, plan.listed
    rows = n * plan.send
    upper = onehot(iota((h, h), 0) < iota((h, h), 1))
    peer_ids = iota((n, h), 0)
    owners = [owner_ref[s : s + 1, :] for s in range(plan.snaps)]
    marks = jnp.concatenate([onehot(peer_ids == o) for o in owners], axis=0)
    prefix = dot(marks, upper, 1, 0)
    row_ids = iota((rows, h), 0)
    list_ids = iota((k, h), 0)
    for g in range(plan.groups):
        acc = jnp.zeros((rows, plan.width), jnp.float32)
        for q in range(plan.per):
            s = g * plan.per + q
            mine = jnp.where(peer_ids == owners[s], prefix[s * n : (s + 1) * n], 0.0)
            rank = jnp.sum(mine, axis=0, keepdims=True).astype(jnp.int32)
            live = live_ref[s : s + 1, :] == 1
            place = q * plan.slots + rank
            target_ref[s : s + 1, :] = jnp.where(live, owners[s] * LANES + place, -LANES)
            listing = cand_ref[s]
            pick = pick_ref[s : s + 1, :]
            chosen = jnp.sum(jnp.where(list_ids == pick, listing, 0), axis=0, keepdims=True)
            first = listing[0:1, :]
            kept = jnp.where(list_ids < span_ref[s : s + 1, :], listing, chosen)
            kept = jnp.where(list_ids == pick, first, kept)
            kept = jnp.where(list_ids == 0, chosen, kept)
            code = jnp.where(kept < plan.half, kept - plan.half, kept - plan.half + 1)
            code = code.astype(jnp.float32)
            spot = place % plan.fit
            spread = jnp.concatenate(
                [jnp.where(spot == b, code, 0.0) for b in range(plan.fit)], axis=0
            ).astype(jnp.bfloat16)
            data_row = jnp.where(live, owners[s] * plan.send + place, -1)
            meta_row = jnp.where(live, owners[s] * plan.send + plan.data + place // plan.fit, -1)
            acc += dot(onehot(row_ids == data_row), rows_ref[s], 1, 0)
            acc += dot(onehot(row_ids == meta_row), spread, 1, 1)
        out_ref[:, g] = acc.astype(jnp.bfloat16).reshape(n, plan.send, plan.width)


def soft(v):
    return 1.0 + (jnp.maximum(v, 0.0) + jnp.log1p(jnp.exp(-jnp.abs(v))))


def owner_kernel(plan, rep_ref, got_ref, own_ref, other_ref, out_ref):
    n, t, c, k = plan.peers, plan.total, plan.cands, plan.listed
    rep = rep_ref[0]
    scale = 1.0 / math.sqrt(plan.width * plan.groups)
    lane = iota((t, LANES), 1)
    slot_ids = iota((t, 1), 0)
    slot = slot_ids % plan.slots
    source = slot_ids // plan.slots
    col = iota((1, c), 1)
    code = jnp.where(col < plan.half, col - plan.half, col - plan.half + 1).astype(jnp.float32)
    fold = onehot(iota((LANES, k), 0) % k == iota((LANES, k), 1))
    if plan.aligned:
        meta = got_ref[:, 0, plan.data : plan.send, :]
        tall, start = plan.send - plan.data, 0
    else:
        meta = got_ref[:, 0]
        tall, start = plan.send, plan.data
    meta = meta.reshape(n * tall, LANES)
    lanes_of = iota((t, n * tall), 1)
    best_parts = []
    blends = []
    for q in range(plan.per):
        place = q * plan.slots + slot
        pull = onehot(lanes_of == source * tall + start + place // plan.fit)
        wide = dot(pull, meta, 1, 0)
        wide = jnp.where(lane // k == place % plan.fit, wide, 0.0).astype(jnp.bfloat16)
        codes = dot(wide, fold, 1, 0)

        def rows_of(r):
            if plan.aligned:
                piece = got_ref[:, r, q * plan.slots : (q + 1) * plan.slots, :]
                return piece.reshape(t, plan.width)
            whole = got_ref[:, r].reshape(n * plan.send, plan.width)
            take = onehot(iota((t, n * plan.send), 1) == source * plan.send + place)
            return dot(take, whole, 1, 0).astype(jnp.bfloat16)

        rows_own, rows_other = rows_of(rep), rows_of(1 - rep)
        own, other = own_ref[q], other_ref[q]
        merit = (dot(rows_own, own, 1, 1) + dot(rows_other, other, 1, 1)) * scale
        chosen = codes[:, 0:1] == code
        mask = chosen
        for j in range(1, k):
            mask = mask | (codes[:, j : j + 1] == code)
        listed = jnp.where(mask, merit, NEG)
        best = jnp.max(listed, axis=1, keepdims=True)
        top = jnp.max(listed, axis=0, keepdims=True)
        picked = jnp.sum(jnp.where(chosen, merit, 0.0), axis=1, keepdims=True)
        rival = jnp.sum(jnp.where(chosen, top, 0.0), axis=1, keepdims=True)
        mine, claim = soft(picked), soft(rival)
        share = mine / (mine + claim)
        select = onehot(chosen)
        pair = []
        for rows, table in ((rows_own, own), (rows_other, other)):
            desc = dot(select, table, 1, 0)
            pair.append(((1.0 - share) * rows.astype(jnp.float32) + share * desc).astype(jnp.bfloat16))
        blends.append(pair)
        best_parts.append(jnp.where(lane == place, best, 0.0).astype(jnp.bfloat16))
    bests = jnp.concatenate(best_parts, axis=0)
    if plan.aligned:
        tall, start = plan.back - plan.data, 0
    else:
        tall, start = plan.back, plan.data
    where_to = iota((n * tall, plan.per * t), 0)
    source_of = (iota((n * tall, plan.per * t), 1) % t) // plan.slots
    tail = dot(onehot(where_to == source_of * tall + start), bests, 1, 0)
    for i, r in enumerate((rep, 1 - rep)):
        if plan.aligned:
            for q in range(plan.per):
                out_ref[:, r, q * plan.slots : (q + 1) * plan.slots, :] = blends[q][i].reshape(
                    n, plan.slots, plan.width
                )
            out_ref[:, r, plan.data : plan.back, :] = tail.astype(jnp.bfloat16).reshape(n, tall, LANES)
        else:
            both = jnp.concatenate([blends[q][i] for q in range(plan.per)], axis=0)
            item = iota((n * tall, plan.per * t), 1)
            spot = ((item % t) // plan.slots) * tall + (item // t) * plan.slots + item % plan.slots
            full = tail + dot(onehot(where_to == spot), both, 1, 0)
            out_ref[:, r] = full.astype(jnp.bfloat16).reshape(n, tall, LANES)


def land_kernel(plan, back_ref, target_ref, rows_ref, out_ref, best_ref):
    n, h = plan.peers, plan.halos
    tall = n * plan.back
    target = target_ref[...]
    column = jnp.transpose(target)
    if plan.aligned:
        short, start = plan.back - plan.data, 0
    else:
        short, start = plan.back, plan.data
    same = iota((h, h), 0) == iota((h, h), 1)
    for g in range(plan.groups):
        whole = back_ref[:, g].reshape(tall, plan.width)
        if plan.aligned:
            tail = back_ref[:, g, plan.data : plan.back, :].reshape(n * short, LANES)
        else:
            tail = whole
        for q in range(plan.per):
            s = g * plan.per + q
            spot = column[:, s : s + 1]
            owner, place = spot // LANES, spot % LANES
            take = onehot(iota((h, tall), 1) == jnp.where(spot >= 0, owner * plan.back + place, -1))
            keep = onehot(same & (spot < 0))
            out_ref[s] = (dot(take, whole, 1, 0) + dot(keep, rows_ref[s], 1, 0)).astype(jnp.bfloat16)
            spot = target[s : s + 1, :]
            owner, place = spot // LANES, spot % LANES
            pull = onehot(iota((n * short, h), 0) == jnp.where(spot >= 0, owner * short + start, -1))
            grid = dot(tail, pull, 0, 0)
            grid = jnp.where(iota((LANES, h), 0) == place, grid, 0.0)
            best_ref[s : s + 1, :] = jnp.sum(grid, axis=0, keepdims=True).astype(jnp.bfloat16)


def body(halo_rows, unmatched, owner_id, cand_index, lengths, choice_index, desc_rows):
    peers, groups = lax.axis_size("space"), lax.axis_size("rep")
    snaps, halos, width = halo_rows.shape
    cands, listed = desc_rows.shape[1], cand_index.shape[2]
    plan = Plan(peers, groups, snaps, halos, width, cands, listed)
    rep = lax.axis_index("rep").astype(jnp.int32)
    per = plan.per

    other_part = lax.dynamic_slice_in_dim(desc_rows, (1 - rep) * per, per, 0)
    other = lax.ppermute(other_part, "rep", [(0, 1), (1, 0)])
    own = lax.dynamic_slice_in_dim(desc_rows, rep * per, per, 0)

    vmem = pl.BlockSpec(memory_space=pltpu.VMEM)
    smem = pl.BlockSpec(memory_space=pltpu.SMEM)
    sent, target = pl.pallas_call(
        lambda *refs: route_kernel(plan, *refs),
        name="route",
        out_shape=(
            jax.ShapeDtypeStruct((peers, groups, plan.send, width), jnp.bfloat16),
            jax.ShapeDtypeStruct((snaps, halos), jnp.int32),
        ),
        in_specs=[vmem] * 6,
        out_specs=(vmem, vmem),
    )(
        owner_id.reshape(snaps, halos),
        unmatched,
        jnp.swapaxes(cand_index, 1, 2),
        lengths,
        choice_index,
        halo_rows,
    )
    got = lax.all_to_all(
        sent.reshape(peers * groups, plan.send, width), ("space", "rep"), 0, 0, tiled=True
    ).reshape(peers, groups, plan.send, width)
    reply = pl.pallas_call(
        lambda *refs: owner_kernel(plan, *refs),
        name="owner",
        out_shape=jax.ShapeDtypeStruct((peers, groups, plan.back, width), jnp.bfloat16),
        in_specs=[smem, vmem, vmem, vmem],
        out_specs=vmem,
    )(rep.reshape(1), got, own, other)
    back = lax.all_to_all(
        reply.reshape(peers * groups, plan.back, width), ("space", "rep"), 0, 0, tiled=True
    ).reshape(peers, groups, plan.back, width)
    return pl.pallas_call(
        lambda *refs: land_kernel(plan, *refs),
        name="land",
        out_shape=(
            jax.ShapeDtypeStruct((snaps, halos, width), jnp.bfloat16),
            jax.ShapeDtypeStruct((snaps, halos), jnp.bfloat16),
        ),
        in_specs=[vmem] * 3,
        out_specs=(vmem, vmem),
    )(back, target, halo_rows)


def solution(mesh):
    in_specs = (
        P(None, "space", "rep"),
        P(None, "space"),
        P(None, "space", None),
        P(None, "space", None),
        P(None, "space"),
        P(None, "space"),
        P(None, "space", "rep"),
    )
    out_specs = (P(None, "space", "rep"), P(None, "space"))
    return jax.shard_map(body, mesh=mesh, in_specs=in_specs, out_specs=out_specs, check_vma=False)
```

```python
import math

import jax
import jax.numpy as jnp
from jax import lax
from jax.experimental import pallas as pl
from jax.experimental.pallas import tpu as pltpu
from jax.sharding import PartitionSpec as P

LANES = 128
SUB = 8
WORD = 32
NEG = -3.0e38


def iota(shape, axis):
    return lax.broadcasted_iota(jnp.int32, shape, axis)


def over(x, m):
    return x >> (m.bit_length() - 1) if m & (m - 1) == 0 else x // m


def left(x, m):
    return x & (m - 1) if m & (m - 1) == 0 else x % m


def onehot(mask):
    return jnp.where(mask, 1.0, 0.0).astype(jnp.bfloat16)


def dot(a, b, ca, cb):
    return lax.dot_general(a, b, (((ca,), (cb,)), ((), ())), preferred_element_type=jnp.float32)


class Plan:
    def __init__(self, peers, groups, snaps, halos, width, cands, listed):
        self.peers, self.groups, self.snaps = peers, groups, snaps
        self.halos, self.width, self.cands, self.listed = halos, width, cands, listed
        self.per = snaps // groups
        self.slots = 2 * halos // peers
        self.total = peers * self.slots
        self.data = self.per * self.slots
        self.fit = LANES // listed
        self.codes = -(-(-(-self.data // self.fit)) // groups)
        self.send = self.data + self.codes + (self.data + self.codes) % 2
        self.back = self.data + 1 + (self.data + 1) % 2
        self.half = cands // 2
        self.aligned = self.slots % SUB == 0
        assert snaps % groups == 0 and groups == 2
        assert width == LANES and halos <= LANES and cands <= 512 and cands % WORD == 0
        assert LANES % listed == 0 and self.data <= LANES
        assert peers * groups * self.send % SUB == 0 and peers * groups * self.back % SUB == 0
        assert not self.aligned or (self.codes <= SUB <= self.data)

    def at(self, peer, group, size):
        return (peer * self.groups + group) * size


def route_kernel(plan, rep_ref, owner_ref, live_ref, cand_ref, span_ref, pick_ref, rows_ref, out_ref, target_ref):
    n, h, k = plan.peers, plan.halos, plan.listed
    rep = rep_ref[0]
    upper = onehot(iota((h, h), 0) < iota((h, h), 1))
    peer_ids = iota((n, h), 0)
    owners = [owner_ref[s : s + 1, :] for s in range(plan.snaps)]
    marks = jnp.concatenate([onehot(peer_ids == o) for o in owners], axis=0)
    prefix = dot(marks, upper, 1, 0)
    list_ids = iota((k, h), 0)
    whole = None
    for g in range(plan.groups):
        rows, tail = None, None
        for q in range(plan.per):
            s = g * plan.per + q
            mine = jnp.where(peer_ids == owners[s], prefix[s * n : (s + 1) * n], 0.0)
            rank = jnp.sum(mine, axis=0, keepdims=True).astype(jnp.int32)
            live = live_ref[s : s + 1, :] == 1
            place = q * plan.slots + rank
            target_ref[s : s + 1, :] = jnp.where(live, owners[s] * LANES + place, -LANES)
            listing = cand_ref[s]
            pick = pick_ref[s : s + 1, :]
            chosen = jnp.sum(jnp.where(list_ids == pick, listing, 0), axis=0, keepdims=True)
            first = listing[0:1, :]
            kept = jnp.where(list_ids < span_ref[s : s + 1, :], listing, chosen)
            kept = jnp.where(list_ids == pick, first, kept)
            kept = jnp.where(list_ids == 0, chosen, kept)
            code = jnp.where(kept < plan.half, kept - plan.half, kept - plan.half + 1)
            code = code.astype(jnp.float32)
            spot, line = left(place, plan.fit), over(place, plan.fit)
            spread = jnp.concatenate(
                [jnp.where(spot == b, code, 0.0) for b in range(plan.fit)], axis=0
            ).astype(jnp.bfloat16)
            tells = live & (over(line, plan.codes) == rep)
            line = left(line, plan.codes)
            if plan.aligned:
                put = iota((n * plan.data, h), 0) == jnp.where(live, owners[s] * plan.data + place, -1)
                say = iota((n * SUB, h), 0) == jnp.where(tells, owners[s] * SUB + line, -1)
            else:
                base = plan.at(owners[s], g, plan.send)
                ids = iota((n * plan.groups * plan.send, h), 0)
                put = ids == jnp.where(live, base + place, -1)
                say = ids == jnp.where(tells, base + plan.data + line, -1)
            part = dot(onehot(put), rows_ref[s], 1, 0)
            note = dot(onehot(say), spread, 1, 1)
            rows = part if rows is None else rows + part
            tail = note if tail is None else tail + note
        if plan.aligned:
            rows, tail = rows.astype(jnp.bfloat16), tail.astype(jnp.bfloat16)
            for p in range(n):
                base = plan.at(p, g, plan.send)
                out_ref[base : base + plan.data, :] = rows[p * plan.data : (p + 1) * plan.data]
                out_ref[base + plan.data : base + plan.send, :] = tail[p * SUB : p * SUB + plan.send - plan.data]
        else:
            both = rows + tail
            whole = both if whole is None else whole + both
    if not plan.aligned:
        out_ref[...] = whole.astype(jnp.bfloat16)


def soft(v):
    return 1.0 + (jnp.maximum(v, 0.0) + jnp.log1p(jnp.exp(-jnp.abs(v))))


def rows_in(plan, ref, group, q, size):
    if plan.aligned:
        starts = [plan.at(p, group, size) + q * plan.slots for p in range(plan.peers)]
        return jnp.concatenate([ref[a : a + plan.slots, :] for a in starts], axis=0)
    shape = (plan.total, plan.peers * plan.groups * size)
    item = iota(shape, 0)
    spot = plan.at(over(item, plan.slots), group, size) + q * plan.slots + left(item, plan.slots)
    return dot(onehot(iota(shape, 1) == spot), ref[...], 1, 0).astype(jnp.bfloat16)


def tail_in(plan, ref, group, size):
    if plan.aligned:
        ends = [plan.at(p, group, size) + size for p in range(plan.peers)]
        value = jnp.concatenate([ref[a - SUB : a, :] for a in ends], axis=0)
        return value, (lambda p: p * SUB + SUB - (size - plan.data))
    return ref[...], (lambda p: plan.at(p, group, size) + plan.data)


def owner_kernel(plan, rep_ref, got_ref, own_ref, other_ref, out_ref):
    n, t, c, k = plan.peers, plan.total, plan.cands, plan.listed
    first = rep_ref[0] == 0
    scale = 1.0 / math.sqrt(plan.width * plan.groups)
    item = iota((1, t), 1)
    source, slot = over(item, plan.slots), left(item, plan.slots)
    snaps, cores = range(plan.per), range(plan.groups)
    ends = [tail_in(plan, got_ref, r, plan.send) for r in cores]

    listing = []
    for q in snaps:
        place = q * plan.slots + slot
        spot, line = left(place, plan.fit), over(place, plan.fit)
        wide = None
        for r in cores:
            value, row = ends[r]
            if (q * plan.slots + plan.slots - 1) // plan.fit // plan.codes < r:
                continue
            if q * plan.slots // plan.fit // plan.codes > r:
                continue
            told = jnp.where(over(line, plan.codes) == r, row(source) + left(line, plan.codes), -1)
            piece = dot(value, onehot(iota((value.shape[0], t), 0) == told), 0, 0)
            wide = piece if wide is None else wide + piece
        codes = None
        for b in range(plan.fit):
            piece = jnp.where(spot == b, wide[b * k : (b + 1) * k], 0.0)
            codes = piece if codes is None else codes + piece
        codes = codes.astype(jnp.int32)
        index = jnp.where(codes < 0, codes + plan.half, codes + plan.half - 1)
        listing.append(jnp.where(codes == 0, -1, index))

    tables = [
        [jnp.where(first, own_ref[q], other_ref[q]), jnp.where(first, other_ref[q], own_ref[q])] for q in snaps
    ]
    rows = [[rows_in(plan, got_ref, r, q, plan.send) for r in cores] for q in snaps]
    merits = [sum(dot(tables[q][r], rows[q][r], 1, 1) for r in cores) for q in snaps]

    words = c // WORD
    word_ids = iota((words, t), 0)
    bits = jnp.left_shift(jnp.int32(1), iota((WORD, t), 0))
    heads = [listing[q][0:1, :].astype(jnp.float32) for q in snaps]
    heads = jnp.transpose(jnp.concatenate(heads + [jnp.zeros((SUB - plan.per, t), jnp.float32)], axis=0))
    heads = heads.astype(jnp.int32)
    bests, shares = [], []
    for q in snaps:
        index = listing[q]
        high, bit = index >> 5, jnp.left_shift(jnp.int32(1), index & (WORD - 1))
        sets = jnp.zeros((words, t), jnp.int32)
        for j in range(k):
            sets = sets | jnp.where(high[j : j + 1, :] == word_ids, bit[j : j + 1, :], 0)
        parts = []
        for w in range(words):
            member = (sets[w : w + 1, :] & bits) != 0
            parts.append(jnp.where(member, merits[q][w * WORD : (w + 1) * WORD], NEG))
        listed = jnp.concatenate(parts, axis=0)
        bests.append(jnp.max(listed, axis=0, keepdims=True) * scale)
        top = jnp.max(listed, axis=1, keepdims=True)
        chosen = iota((c, t), 0) == index[0:1, :]
        picked = jnp.sum(jnp.where(chosen, merits[q], 0.0), axis=0, keepdims=True) * scale
        rival = jnp.sum(jnp.where(chosen, top, 0.0), axis=0, keepdims=True) * scale
        mine, claim = soft(picked), soft(rival)
        shares.append(mine / (mine + claim))
    shares = jnp.transpose(jnp.concatenate(shares + [jnp.zeros((SUB - plan.per, t), jnp.float32)], axis=0))

    blends = []
    for q in snaps:
        select = onehot(iota((t, c), 1) == heads[:, q : q + 1])
        share = shares[:, q : q + 1]
        pair = []
        for r in cores:
            desc = dot(select, tables[q][r], 1, 0)
            pair.append(((1.0 - share) * rows[q][r].astype(jnp.float32) + share * desc).astype(jnp.bfloat16))
        blends.append(pair)

    tail = None
    lane = iota((t, LANES), 1)
    for q in snaps:
        if plan.aligned:
            shape = (n * SUB, t)
            home = source * SUB
        else:
            shape = (n * plan.back, t)
            home = source * plan.back + plan.data
        line = jnp.where(iota(shape, 0) == home, jnp.maximum(bests[q], NEG), 0.0).astype(jnp.bfloat16)
        piece = dot(line, onehot(lane == q * plan.slots + left(iota((t, LANES), 0), plan.slots)), 1, 0)
        tail = piece if tail is None else tail + piece
    if plan.aligned:
        tail = tail.astype(jnp.bfloat16)
        for r in cores:
            for p in range(n):
                base = plan.at(p, r, plan.back)
                for q in snaps:
                    a = base + q * plan.slots
                    out_ref[a : a + plan.slots, :] = blends[q][r][p * plan.slots : (p + 1) * plan.slots]
                out_ref[base + plan.data : base + plan.back, :] = tail[p * SUB : p * SUB + plan.back - plan.data]
        return
    shape = (n * plan.groups * plan.back, t)
    item = iota(shape, 1)
    peer, slot = over(item, plan.slots), left(item, plan.slots)
    shape_tail = (n * plan.groups * plan.back, n * plan.back)
    row, col = iota(shape_tail, 0), iota(shape_tail, 1)
    peer_of, line_of = col // plan.back, col % plan.back
    full = None
    for r in cores:
        copy = onehot(row == plan.at(peer_of, r, plan.back) + line_of)
        piece = dot(copy, tail.astype(jnp.bfloat16), 1, 0)
        for q in snaps:
            put = onehot(iota(shape, 0) == plan.at(peer, r, plan.back) + q * plan.slots + slot)
            piece = piece + dot(put, blends[q][r], 1, 0)
        full = piece if full is None else full + piece
    out_ref[...] = full.astype(jnp.bfloat16)


def land_kernel(plan, back_ref, target_ref, rows_ref, out_ref, best_ref):
    h = plan.halos
    target = target_ref[...]
    column = jnp.transpose(target)
    same = iota((h, h), 0) == iota((h, h), 1)
    for g in range(plan.groups):
        tail, row = tail_in(plan, back_ref, g, plan.back)
        for q in range(plan.per):
            s = g * plan.per + q
            spot = column[:, s : s + 1]
            owner, slot = spot >> 7, (spot & (LANES - 1)) - q * plan.slots
            rows = rows_in(plan, back_ref, g, q, plan.back)
            where_from = jnp.where(spot >= 0, owner * plan.slots + slot, -1)
            take = onehot(iota((h, plan.total), 1) == where_from)
            keep = onehot(same & (spot < 0))
            out_ref[s] = (dot(take, rows, 1, 0) + dot(keep, rows_ref[s], 1, 0)).astype(jnp.bfloat16)
            spot = target[s : s + 1, :]
            owner, place = spot >> 7, spot & (LANES - 1)
            pull = onehot(iota((tail.shape[0], h), 0) == jnp.where(spot >= 0, row(owner), -1))
            grid = dot(tail, pull, 0, 0)
            grid = jnp.where(iota((LANES, h), 0) == place, grid, 0.0)
            best_ref[s : s + 1, :] = jnp.sum(grid, axis=0, keepdims=True).astype(jnp.bfloat16)


def body(halo_rows, unmatched, owner_id, cand_index, lengths, choice_index, desc_rows):
    peers, groups = lax.axis_size("space"), lax.axis_size("rep")
    snaps, halos, width = halo_rows.shape
    cands, listed = desc_rows.shape[1], cand_index.shape[2]
    plan = Plan(peers, groups, snaps, halos, width, cands, listed)
    rep = lax.axis_index("rep").astype(jnp.int32)
    per = plan.per

    def swap(flat, size):
        boxed = flat.reshape(peers * groups, size // 2, 2, width)
        boxed = lax.all_to_all(boxed, ("space", "rep"), 0, 0, tiled=True)
        return boxed.reshape(peers * groups * size, width)

    other_part = lax.dynamic_slice_in_dim(desc_rows, (1 - rep) * per, per, 0)
    other = lax.ppermute(other_part, "rep", [(0, 1), (1, 0)])
    own = lax.dynamic_slice_in_dim(desc_rows, rep * per, per, 0)

    vmem = pl.BlockSpec(memory_space=pltpu.VMEM)
    smem = pl.BlockSpec(memory_space=pltpu.SMEM)
    small = pltpu.CompilerParams(vmem_limit_bytes=20 << 20)
    sent, target = pl.pallas_call(
        lambda *refs: route_kernel(plan, *refs),
        name="route",
        out_shape=(
            jax.ShapeDtypeStruct((peers * groups * plan.send, width), jnp.bfloat16),
            jax.ShapeDtypeStruct((snaps, halos), jnp.int32),
        ),
        in_specs=[smem] + [vmem] * 6,
        out_specs=(vmem, vmem),
    )(
        rep.reshape(1),
        owner_id.reshape(snaps, halos),
        unmatched,
        jnp.swapaxes(cand_index, 1, 2),
        lengths,
        choice_index,
        halo_rows,
    )
    got = swap(sent, plan.send)
    reply = pl.pallas_call(
        lambda *refs: owner_kernel(plan, *refs),
        name="owner",
        compiler_params=small,
        out_shape=jax.ShapeDtypeStruct((peers * groups * plan.back, width), jnp.bfloat16),
        in_specs=[smem, vmem, vmem, vmem],
        out_specs=vmem,
    )(rep.reshape(1), got, own, other)
    back = swap(reply, plan.back)
    return pl.pallas_call(
        lambda *refs: land_kernel(plan, *refs),
        name="land",
        compiler_params=small,
        out_shape=(
            jax.ShapeDtypeStruct((snaps, halos, width), jnp.bfloat16),
            jax.ShapeDtypeStruct((snaps, halos), jnp.bfloat16),
        ),
        in_specs=[vmem] * 3,
        out_specs=(vmem, vmem),
    )(back, target, halo_rows)


def solution(mesh):
    in_specs = (
        P(None, "space", "rep"),
        P(None, "space"),
        P(None, "space", None),
        P(None, "space", None),
        P(None, "space"),
        P(None, "space"),
        P(None, "space", "rep"),
    )
    out_specs = (P(None, "space", "rep"), P(None, "space"))
    return jax.shard_map(body, mesh=mesh, in_specs=in_specs, out_specs=out_specs, check_vma=False)
```

```python
import math

import jax
import jax.numpy as jnp
from jax import lax
from jax.experimental import pallas as pl
from jax.experimental.pallas import tpu as pltpu
from jax.sharding import PartitionSpec as P

LANES = 128
SUB = 8
WORD = 32
NEG = -3.0e38


def iota(shape, axis):
    return lax.broadcasted_iota(jnp.int32, shape, axis)


def over(x, m):
    return x >> (m.bit_length() - 1) if m & (m - 1) == 0 else x // m


def left(x, m):
    return x & (m - 1) if m & (m - 1) == 0 else x % m


def onehot(mask):
    return jnp.where(mask, 1.0, 0.0).astype(jnp.bfloat16)


def dot(a, b, ca, cb):
    return lax.dot_general(a, b, (((ca,), (cb,)), ((), ())), preferred_element_type=jnp.float32)


class Plan:
    def __init__(self, peers, groups, snaps, halos, width, cands, listed):
        self.peers, self.groups, self.snaps = peers, groups, snaps
        self.halos, self.width, self.cands, self.listed = halos, width, cands, listed
        self.per = snaps // groups
        self.slots = 2 * halos // peers
        self.total = peers * self.slots
        self.data = self.per * self.slots
        self.fit = LANES // listed
        self.codes = -(-(-(-self.data // self.fit)) // groups)
        self.send = self.data + self.codes + (self.data + self.codes) % 2
        self.back = self.data + 1 + (self.data + 1) % 2
        self.half = cands // 2
        self.aligned = self.slots % SUB == 0
        assert snaps % groups == 0 and groups == 2
        assert width == LANES and halos <= LANES and cands <= 512 and cands % WORD == 0
        assert LANES % listed == 0 and self.data <= LANES
        assert peers * groups * self.send % SUB == 0 and peers * groups * self.back % SUB == 0
        assert not self.aligned or (self.codes <= SUB <= self.data)

    def at(self, peer, group, size):
        return (peer * self.groups + group) * size


def route_kernel(plan, rep_ref, *refs):
    sources, (out_ref, target_ref), held = refs[:6], refs[6:8], refs[8:14]
    sems = refs[14]
    copies = [pltpu.make_async_copy(x, y, sems.at[i]) for i, (x, y) in enumerate(zip(sources, held))]
    for copy in copies:
        copy.start()
    owner_ref, live_ref, cand_ref, span_ref, pick_ref, rows_ref = held
    n, h, k = plan.peers, plan.halos, plan.listed
    rep = rep_ref[0]
    upper = onehot(iota((h, h), 0) < iota((h, h), 1))
    peer_ids = iota((n, h), 0)
    list_ids = iota((k, h), 0)
    for copy in copies[:-1]:
        copy.wait()
    owners = [owner_ref[s : s + 1, :] for s in range(plan.snaps)]
    marks = jnp.concatenate([onehot(peer_ids == o) for o in owners], axis=0)
    prefix = dot(marks, upper, 1, 0)
    puts, says, spreads = [], [], []
    for s in range(plan.snaps):
        g, q = s // plan.per, s % plan.per
        mine = jnp.where(peer_ids == owners[s], prefix[s * n : (s + 1) * n], 0.0)
        rank = jnp.sum(mine, axis=0, keepdims=True).astype(jnp.int32)
        live = live_ref[s : s + 1, :] == 1
        place = q * plan.slots + rank
        target_ref[s : s + 1, :] = jnp.where(live, owners[s] * LANES + place, -LANES)
        listing = cand_ref[s]
        pick = pick_ref[s : s + 1, :]
        chosen = jnp.sum(jnp.where(list_ids == pick, listing, 0), axis=0, keepdims=True)
        first = listing[0:1, :]
        kept = jnp.where(list_ids < span_ref[s : s + 1, :], listing, chosen)
        kept = jnp.where(list_ids == pick, first, kept)
        kept = jnp.where(list_ids == 0, chosen, kept)
        code = jnp.where(kept < plan.half, kept - plan.half, kept - plan.half + 1)
        code = code.astype(jnp.float32)
        spot, line = left(place, plan.fit), over(place, plan.fit)
        spread = jnp.concatenate([jnp.where(spot == b, code, 0.0) for b in range(plan.fit)], axis=0)
        spreads.append(spread.astype(jnp.bfloat16))
        tells = live & (over(line, plan.codes) == rep)
        line = left(line, plan.codes)
        if plan.aligned:
            put = iota((n * plan.data, h), 0) == jnp.where(live, owners[s] * plan.data + place, -1)
            say = iota((n * SUB, h), 0) == jnp.where(tells, owners[s] * SUB + line, -1)
        else:
            base = plan.at(owners[s], g, plan.send)
            ids = iota((n * plan.groups * plan.send, h), 0)
            put = ids == jnp.where(live, base + place, -1)
            say = ids == jnp.where(tells, base + plan.data + line, -1)
        puts.append(onehot(put))
        says.append(onehot(say))
    tails = []
    for g in range(plan.groups):
        mine = range(g * plan.per, (g + 1) * plan.per)
        tails.append(sum(dot(says[s], spreads[s], 1, 1) for s in mine))
    copies[-1].wait()
    whole = None
    for g in range(plan.groups):
        mine = range(g * plan.per, (g + 1) * plan.per)
        rows = sum(dot(puts[s], rows_ref[s], 1, 0) for s in mine)
        if plan.aligned:
            rows, tail = rows.astype(jnp.bfloat16), tails[g].astype(jnp.bfloat16)
            for p in range(n):
                base = plan.at(p, g, plan.send)
                out_ref[base : base + plan.data, :] = rows[p * plan.data : (p + 1) * plan.data]
                out_ref[base + plan.data : base + plan.send, :] = tail[p * SUB : p * SUB + plan.send - plan.data]
        else:
            both = rows + tails[g]
            whole = both if whole is None else whole + both
    if not plan.aligned:
        out_ref[...] = whole.astype(jnp.bfloat16)


def soft(v):
    return 1.0 + (jnp.maximum(v, 0.0) + jnp.log1p(jnp.exp(-jnp.abs(v))))


def rows_in(plan, ref, group, q, size):
    if plan.aligned:
        starts = [plan.at(p, group, size) + q * plan.slots for p in range(plan.peers)]
        return jnp.concatenate([ref[a : a + plan.slots, :] for a in starts], axis=0)
    shape = (plan.total, plan.peers * plan.groups * size)
    item = iota(shape, 0)
    spot = plan.at(over(item, plan.slots), group, size) + q * plan.slots + left(item, plan.slots)
    return dot(onehot(iota(shape, 1) == spot), ref[...], 1, 0).astype(jnp.bfloat16)


def tail_in(plan, ref, group, size):
    if plan.aligned:
        ends = [plan.at(p, group, size) + size for p in range(plan.peers)]
        value = jnp.concatenate([ref[a - SUB : a, :] for a in ends], axis=0)
        return value, (lambda p: p * SUB + SUB - (size - plan.data))
    return ref[...], (lambda p: plan.at(p, group, size) + plan.data)


def owner_kernel(plan, rep_ref, got_ref, own_ref, other_ref, out_ref):
    n, t, c, k = plan.peers, plan.total, plan.cands, plan.listed
    rep = rep_ref[0]
    scale = 1.0 / math.sqrt(plan.width * plan.groups)
    item = iota((1, t), 1)
    source, slot = over(item, plan.slots), left(item, plan.slots)
    snaps, cores = range(plan.per), range(plan.groups)
    ends = [tail_in(plan, got_ref, r, plan.send) for r in cores]

    listing = []
    for q in snaps:
        place = q * plan.slots + slot
        spot, line = left(place, plan.fit), over(place, plan.fit)
        wide = None
        for r in cores:
            value, row = ends[r]
            if (q * plan.slots + plan.slots - 1) // plan.fit // plan.codes < r:
                continue
            if q * plan.slots // plan.fit // plan.codes > r:
                continue
            told = jnp.where(over(line, plan.codes) == r, row(source) + left(line, plan.codes), -1)
            piece = dot(value, onehot(iota((value.shape[0], t), 0) == told), 0, 0)
            wide = piece if wide is None else wide + piece
        codes = None
        for b in range(plan.fit):
            piece = jnp.where(spot == b, wide[b * k : (b + 1) * k], 0.0)
            codes = piece if codes is None else codes + piece
        codes = codes.astype(jnp.int32)
        index = jnp.where(codes < 0, codes + plan.half, codes + plan.half - 1)
        listing.append(jnp.where(codes == 0, -1, index))

    tables = []
    for q in snaps:
        own, other = own_ref[rep * plan.per + q], other_ref[rep * plan.per + q]
        tables.append([jnp.where(rep == 0, own, other), jnp.where(rep == 0, other, own)])
    rows = [[rows_in(plan, got_ref, r, q, plan.send) for r in cores] for q in snaps]
    merits = [sum(dot(tables[q][r], rows[q][r], 1, 1) for r in cores) for q in snaps]

    words = c // WORD
    word_ids = iota((words, t), 0)
    bits = jnp.left_shift(jnp.int32(1), iota((WORD, t), 0))
    heads = [listing[q][0:1, :].astype(jnp.float32) for q in snaps]
    heads = jnp.transpose(jnp.concatenate(heads + [jnp.zeros((SUB - plan.per, t), jnp.float32)], axis=0))
    heads = heads.astype(jnp.int32)
    bests, shares = [], []
    for q in snaps:
        index = listing[q]
        high, bit = index >> 5, jnp.left_shift(jnp.int32(1), index & (WORD - 1))
        sets = jnp.zeros((words, t), jnp.int32)
        for j in range(k):
            sets = sets | jnp.where(high[j : j + 1, :] == word_ids, bit[j : j + 1, :], 0)
        parts = []
        for w in range(words):
            member = (sets[w : w + 1, :] & bits) != 0
            parts.append(jnp.where(member, merits[q][w * WORD : (w + 1) * WORD], NEG))
        listed = jnp.concatenate(parts, axis=0)
        bests.append(jnp.max(listed, axis=0, keepdims=True) * scale)
        top = jnp.max(listed, axis=1, keepdims=True)
        chosen = iota((c, t), 0) == index[0:1, :]
        picked = jnp.sum(jnp.where(chosen, merits[q], 0.0), axis=0, keepdims=True) * scale
        rival = jnp.sum(jnp.where(chosen, top, 0.0), axis=0, keepdims=True) * scale
        mine, claim = soft(picked), soft(rival)
        shares.append(mine / (mine + claim))
    shares = jnp.transpose(jnp.concatenate(shares + [jnp.zeros((SUB - plan.per, t), jnp.float32)], axis=0))

    blends = []
    for q in snaps:
        select = onehot(iota((t, c), 1) == heads[:, q : q + 1])
        share = shares[:, q : q + 1]
        pair = []
        for r in cores:
            desc = dot(select, tables[q][r], 1, 0)
            pair.append(((1.0 - share) * rows[q][r].astype(jnp.float32) + share * desc).astype(jnp.bfloat16))
        blends.append(pair)

    tail = None
    lane = iota((t, LANES), 1)
    for q in snaps:
        if plan.aligned:
            shape = (n * SUB, t)
            home = source * SUB
        else:
            shape = (n * plan.back, t)
            home = source * plan.back + plan.data
        line = jnp.where(iota(shape, 0) == home, jnp.maximum(bests[q], NEG), 0.0).astype(jnp.bfloat16)
        piece = dot(line, onehot(lane == q * plan.slots + left(iota((t, LANES), 0), plan.slots)), 1, 0)
        tail = piece if tail is None else tail + piece
    if plan.aligned:
        tail = tail.astype(jnp.bfloat16)
        for r in cores:
            for p in range(n):
                base = plan.at(p, r, plan.back)
                for q in snaps:
                    a = base + q * plan.slots
                    out_ref[a : a + plan.slots, :] = blends[q][r][p * plan.slots : (p + 1) * plan.slots]
                out_ref[base + plan.data : base + plan.back, :] = tail[p * SUB : p * SUB + plan.back - plan.data]
        return
    shape = (n * plan.groups * plan.back, t)
    item = iota(shape, 1)
    peer, slot = over(item, plan.slots), left(item, plan.slots)
    shape_tail = (n * plan.groups * plan.back, n * plan.back)
    row, col = iota(shape_tail, 0), iota(shape_tail, 1)
    peer_of, line_of = col // plan.back, col % plan.back
    full = None
    for r in cores:
        copy = onehot(row == plan.at(peer_of, r, plan.back) + line_of)
        piece = dot(copy, tail.astype(jnp.bfloat16), 1, 0)
        for q in snaps:
            put = onehot(iota(shape, 0) == plan.at(peer, r, plan.back) + q * plan.slots + slot)
            piece = piece + dot(put, blends[q][r], 1, 0)
        full = piece if full is None else full + piece
    out_ref[...] = full.astype(jnp.bfloat16)


def land_kernel(plan, back_ref, target_ref, rows_ref, out_ref, best_ref):
    h = plan.halos
    target = target_ref[...]
    column = jnp.transpose(target)
    same = iota((h, h), 0) == iota((h, h), 1)
    for g in range(plan.groups):
        tail, row = tail_in(plan, back_ref, g, plan.back)
        for q in range(plan.per):
            s = g * plan.per + q
            spot = column[:, s : s + 1]
            owner, slot = spot >> 7, (spot & (LANES - 1)) - q * plan.slots
            rows = rows_in(plan, back_ref, g, q, plan.back)
            where_from = jnp.where(spot >= 0, owner * plan.slots + slot, -1)
            take = onehot(iota((h, plan.total), 1) == where_from)
            keep = onehot(same & (spot < 0))
            out_ref[s] = (dot(take, rows, 1, 0) + dot(keep, rows_ref[s], 1, 0)).astype(jnp.bfloat16)
            spot = target[s : s + 1, :]
            owner, place = spot >> 7, spot & (LANES - 1)
            pull = onehot(iota((tail.shape[0], h), 0) == jnp.where(spot >= 0, row(owner), -1))
            grid = dot(tail, pull, 0, 0)
            grid = jnp.where(iota((LANES, h), 0) == place, grid, 0.0)
            best_ref[s : s + 1, :] = jnp.sum(grid, axis=0, keepdims=True).astype(jnp.bfloat16)


def body(halo_rows, unmatched, owner_id, cand_index, lengths, choice_index, desc_rows):
    peers, groups = lax.axis_size("space"), lax.axis_size("rep")
    snaps, halos, width = halo_rows.shape
    cands, listed = desc_rows.shape[1], cand_index.shape[2]
    plan = Plan(peers, groups, snaps, halos, width, cands, listed)
    rep = lax.axis_index("rep").astype(jnp.int32)

    def swap(flat, size):
        boxed = flat.reshape(peers * groups, size // 2, 2, width)
        boxed = lax.all_to_all(boxed, ("space", "rep"), 0, 0, tiled=True)
        return boxed.reshape(peers * groups * size, width)

    other = lax.ppermute(desc_rows, "rep", [(0, 1), (1, 0)])

    vmem = pl.BlockSpec(memory_space=pltpu.VMEM)
    smem = pl.BlockSpec(memory_space=pltpu.SMEM)
    hbm = pl.BlockSpec(memory_space=pltpu.HBM)
    small = pltpu.CompilerParams(vmem_limit_bytes=20 << 20)
    flat = (snaps, halos)
    sent, target = pl.pallas_call(
        lambda *refs: route_kernel(plan, *refs),
        name="route",
        compiler_params=small,
        out_shape=(
            jax.ShapeDtypeStruct((peers * groups * plan.send, width), jnp.bfloat16),
            jax.ShapeDtypeStruct(flat, jnp.int32),
        ),
        in_specs=[smem] + [hbm] * 6,
        out_specs=(vmem, vmem),
        scratch_shapes=[
            pltpu.VMEM(flat, jnp.int32),
            pltpu.VMEM(flat, jnp.int32),
            pltpu.VMEM((snaps, listed, halos), jnp.int32),
            pltpu.VMEM(flat, jnp.int32),
            pltpu.VMEM(flat, jnp.int32),
            pltpu.VMEM((snaps, halos, width), jnp.bfloat16),
            pltpu.SemaphoreType.DMA((6,)),
        ],
    )(
        rep.reshape(1),
        *(
            pltpu.with_memory_space_constraint(x, pltpu.HBM)
            for x in (
                owner_id.reshape(flat),
                unmatched,
                jnp.swapaxes(cand_index, 1, 2),
                lengths,
                choice_index,
                halo_rows,
            )
        ),
    )
    sent, other = lax.optimization_barrier((sent, other))
    got = swap(sent, plan.send)
    reply = pl.pallas_call(
        lambda *refs: owner_kernel(plan, *refs),
        name="owner",
        compiler_params=small,
        out_shape=jax.ShapeDtypeStruct((peers * groups * plan.back, width), jnp.bfloat16),
        in_specs=[smem, vmem, vmem, vmem],
        out_specs=vmem,
    )(rep.reshape(1), got, desc_rows, other)
    back = swap(reply, plan.back)
    return pl.pallas_call(
        lambda *refs: land_kernel(plan, *refs),
        name="land",
        compiler_params=small,
        out_shape=(
            jax.ShapeDtypeStruct((snaps, halos, width), jnp.bfloat16),
            jax.ShapeDtypeStruct((snaps, halos), jnp.bfloat16),
        ),
        in_specs=[vmem] * 3,
        out_specs=(vmem, vmem),
    )(back, target, halo_rows)


def solution(mesh):
    in_specs = (
        P(None, "space", "rep"),
        P(None, "space"),
        P(None, "space", None),
        P(None, "space", None),
        P(None, "space"),
        P(None, "space"),
        P(None, "space", "rep"),
    )
    out_specs = (P(None, "space", "rep"), P(None, "space"))
    return jax.shard_map(body, mesh=mesh, in_specs=in_specs, out_specs=out_specs, check_vma=False)
```

```python
import math

import jax
import jax.numpy as jnp
from jax import lax
from jax.experimental import pallas as pl
from jax.experimental.pallas import tpu as pltpu
from jax.sharding import PartitionSpec as P

LANES = 128
SUB = 8
WORD = 32
NEG = -3.0e38


def iota(shape, axis):
    return lax.broadcasted_iota(jnp.int32, shape, axis)


def over(x, m):
    return x >> (m.bit_length() - 1) if m & (m - 1) == 0 else x // m


def left(x, m):
    return x & (m - 1) if m & (m - 1) == 0 else x % m


def hot(shape, axis, spot):
    mask = lax.broadcasted_iota(jnp.int16, shape, axis) == spot.astype(jnp.int16)
    return jnp.where(mask, jnp.bfloat16(1), jnp.bfloat16(0))


def dot(a, b, ca, cb):
    return lax.dot_general(a, b, (((ca,), (cb,)), ((), ())), preferred_element_type=jnp.float32)


class Plan:
    def __init__(self, peers, groups, snaps, halos, width, cands, listed):
        self.peers, self.groups, self.snaps = peers, groups, snaps
        self.halos, self.width, self.cands, self.listed = halos, width, cands, listed
        self.per = snaps // groups
        self.slots = 2 * halos // peers
        self.total = peers * self.slots
        self.data = self.per * self.slots
        self.fit = LANES // listed
        self.codes = -(-(-(-self.data // self.fit)) // groups)
        self.send = self.data + self.codes + (self.data + self.codes) % 2
        self.back = self.data + 1 + (self.data + 1) % 2
        self.half = cands // 2
        self.aligned = self.slots % SUB == 0
        assert snaps % groups == 0 and groups == 2
        assert width == LANES and halos <= LANES and cands <= 512 and cands % WORD == 0
        assert LANES % listed == 0 and self.data <= LANES
        assert peers * groups * self.send % SUB == 0 and peers * groups * self.back % SUB == 0
        assert not self.aligned or (self.codes <= SUB <= self.data)

    def at(self, peer, group, size):
        return (peer * self.groups + group) * size


def route_kernel(plan, rep_ref, *refs):
    sources, (out_ref, target_ref), held = refs[:6], refs[6:8], refs[8:14]
    sems = refs[14]
    copies = [pltpu.make_async_copy(x, y, sems.at[i]) for i, (x, y) in enumerate(zip(sources, held))]
    for copy in copies:
        copy.start()
    owner_ref, live_ref, cand_ref, span_ref, pick_ref, rows_ref = held
    n, h, k = plan.peers, plan.halos, plan.listed
    rep = rep_ref[0]
    upper = iota((h, h), 0) < iota((h, h), 1)
    upper = jnp.where(upper, 1.0, 0.0).astype(jnp.bfloat16)
    peer_ids = iota((n, h), 0)
    list_ids = iota((k, h), 0)
    for copy in copies[:-1]:
        copy.wait()
    owners = [owner_ref[s : s + 1, :] for s in range(plan.snaps)]
    marks = jnp.concatenate([hot((n, h), 0, o) for o in owners], axis=0)
    prefix = dot(marks, upper, 1, 0)
    puts, says, spreads = [], [], []
    for s in range(plan.snaps):
        g, q = s // plan.per, s % plan.per
        mine = jnp.where(peer_ids == owners[s], prefix[s * n : (s + 1) * n], 0.0)
        rank = jnp.sum(mine, axis=0, keepdims=True).astype(jnp.int32)
        live = live_ref[s : s + 1, :] == 1
        place = q * plan.slots + rank
        target_ref[s : s + 1, :] = jnp.where(live, owners[s] * LANES + place, -LANES)
        listing = cand_ref[s]
        pick = pick_ref[s : s + 1, :]
        chosen = jnp.sum(jnp.where(list_ids == pick, listing, 0), axis=0, keepdims=True)
        first = listing[0:1, :]
        kept = jnp.where(list_ids < span_ref[s : s + 1, :], listing, chosen)
        kept = jnp.where(list_ids == pick, first, kept)
        kept = jnp.where(list_ids == 0, chosen, kept)
        code = jnp.where(kept < plan.half, kept - plan.half, kept - plan.half + 1)
        code = code.astype(jnp.float32).astype(jnp.bfloat16)
        spot, line = left(place, plan.fit).astype(jnp.int16), over(place, plan.fit)
        spreads.append(
            jnp.concatenate(
                [jnp.where(jnp.broadcast_to(spot, (k, h)) == b, code, jnp.bfloat16(0)) for b in range(plan.fit)],
                axis=0,
            )
        )
        tells = live & (over(line, plan.codes) == rep)
        line = left(line, plan.codes)
        if plan.aligned:
            puts.append(hot((n * plan.data, h), 0, jnp.where(live, owners[s] * plan.data + place, -1)))
            says.append(hot((n * SUB, h), 0, jnp.where(tells, owners[s] * SUB + line, -1)))
        else:
            base = plan.at(owners[s], g, plan.send)
            shape = (n * plan.groups * plan.send, h)
            puts.append(hot(shape, 0, jnp.where(live, base + place, -1)))
            says.append(hot(shape, 0, jnp.where(tells, base + plan.data + line, -1)))

    def joined(parts, g, axis):
        return jnp.concatenate(parts[g * plan.per : (g + 1) * plan.per], axis=axis)

    tails = [dot(joined(says, g, 1), joined(spreads, g, 1), 1, 1) for g in range(plan.groups)]
    copies[-1].wait()
    whole = None
    for g in range(plan.groups):
        held_rows = rows_ref[g * plan.per : (g + 1) * plan.per].reshape(plan.per * h, plan.width)
        rows = dot(joined(puts, g, 1), held_rows, 1, 0)
        if plan.aligned:
            rows, tail = rows.astype(jnp.bfloat16), tails[g].astype(jnp.bfloat16)
            for p in range(n):
                base = plan.at(p, g, plan.send)
                out_ref[base : base + plan.data, :] = rows[p * plan.data : (p + 1) * plan.data]
                out_ref[base + plan.data : base + plan.send, :] = tail[p * SUB : p * SUB + plan.send - plan.data]
        else:
            both = rows + tails[g]
            whole = both if whole is None else whole + both
    if not plan.aligned:
        out_ref[...] = whole.astype(jnp.bfloat16)


def soft(v):
    return 1.0 + (jnp.maximum(v, 0.0) + jnp.log1p(jnp.exp(-jnp.abs(v))))


def rows_in(plan, ref, group, q, size):
    if plan.aligned:
        starts = [plan.at(p, group, size) + q * plan.slots for p in range(plan.peers)]
        return jnp.concatenate([ref[a : a + plan.slots, :] for a in starts], axis=0)
    item = iota((plan.total, 1), 0)
    spot = plan.at(over(item, plan.slots), group, size) + q * plan.slots + left(item, plan.slots)
    take = hot((plan.total, plan.peers * plan.groups * size), 1, spot)
    return dot(take, ref[...], 1, 0).astype(jnp.bfloat16)


def tail_in(plan, ref, group, size):
    if plan.aligned:
        ends = [plan.at(p, group, size) + size for p in range(plan.peers)]
        value = jnp.concatenate([ref[a - SUB : a, :] for a in ends], axis=0)
        return value, (lambda p: p * SUB + SUB - (size - plan.data))
    return ref[...], (lambda p: plan.at(p, group, size) + plan.data)


def owner_kernel(plan, rep_ref, got_ref, own_ref, other_ref, out_ref):
    n, t, c, k = plan.peers, plan.total, plan.cands, plan.listed
    rep = rep_ref[0]
    scale = 1.0 / math.sqrt(plan.width * plan.groups)
    item = iota((1, t), 1)
    source, slot = over(item, plan.slots), left(item, plan.slots)
    snaps, cores = range(plan.per), range(plan.groups)
    ends = [tail_in(plan, got_ref, r, plan.send) for r in cores]

    tables, rows, merits = [], [], []
    for q in snaps:
        own, other = own_ref[rep * plan.per + q], other_ref[rep * plan.per + q]
        pair = [jnp.where(rep == 0, own, other), jnp.where(rep == 0, other, own)]
        tables.append(jnp.concatenate(pair, axis=1))
        rows.append(jnp.concatenate([rows_in(plan, got_ref, r, q, plan.send) for r in cores], axis=1))

    listing = []
    for q in snaps:
        place = q * plan.slots + slot
        spot, line = left(place, plan.fit), over(place, plan.fit)
        wide = None
        for r in cores:
            value, row = ends[r]
            if (q * plan.slots + plan.slots - 1) // plan.fit // plan.codes < r:
                continue
            if q * plan.slots // plan.fit // plan.codes > r:
                continue
            told = jnp.where(over(line, plan.codes) == r, row(source) + left(line, plan.codes), -1)
            piece = dot(value, hot((value.shape[0], t), 0, told), 0, 0)
            wide = piece if wide is None else wide + piece
        codes = wide[0:k]
        for b in range(1, plan.fit):
            codes = jnp.where(spot == b, wide[b * k : (b + 1) * k], codes)
        codes = codes.astype(jnp.int32)
        index = jnp.where(codes < 0, codes + plan.half, codes + plan.half - 1)
        listing.append(jnp.where(codes == 0, -1, index))
        merits.append(dot(tables[q], rows[q], 1, 1))

    words = c // WORD
    word_ids = iota((words, t), 0)
    line_ids = iota((WORD, t), 0)
    bits = jnp.left_shift(jnp.int32(1), line_ids)
    filler = jnp.zeros((SUB - plan.per, t), jnp.float32)
    heads = [listing[q][0:1, :].astype(jnp.float32) for q in snaps]
    heads = jnp.transpose(jnp.concatenate(heads + [filler], axis=0)).astype(jnp.int32)
    descs = [dot(hot((t, c), 1, heads[:, q : q + 1]), tables[q], 1, 0) for q in snaps]
    bests, shares = [], []
    for q in snaps:
        index = listing[q]
        high, bit = index >> 5, jnp.left_shift(jnp.int32(1), index & (WORD - 1))
        sets = jnp.zeros((words, t), jnp.int32)
        for j in range(k):
            sets = sets | jnp.where(high[j : j + 1, :] == word_ids, bit[j : j + 1, :], 0)
        head = index[0:1, :]
        best = jnp.full((WORD, t), NEG, jnp.float32)
        picked = jnp.zeros((WORD, t), jnp.float32)
        rival = jnp.zeros((WORD, t), jnp.float32)
        for w in range(words):
            merit = merits[q][w * WORD : (w + 1) * WORD]
            member = (sets[w : w + 1, :] & bits) != 0
            listed = jnp.where(member, merit, NEG)
            best = jnp.maximum(best, listed)
            top = jnp.max(listed, axis=1, keepdims=True)
            chosen = line_ids == head - w * WORD
            picked = jnp.where(chosen, merit, picked)
            rival = jnp.where(chosen, top, rival)
        bests.append((jnp.max(best, axis=0, keepdims=True) * scale).astype(jnp.bfloat16))
        mine = soft(jnp.sum(picked, axis=0, keepdims=True) * scale)
        claim = soft(jnp.sum(rival, axis=0, keepdims=True) * scale)
        shares.append(mine / (mine + claim))
    shares = jnp.transpose(jnp.concatenate(shares + [filler], axis=0))

    blends = []
    for q in snaps:
        share = shares[:, q : q + 1]
        blend = (1.0 - share) * rows[q].astype(jnp.float32) + share * descs[q]
        blends.append(blend.astype(jnp.bfloat16))

    tall = SUB if plan.aligned else plan.back
    home = source * tall + (0 if plan.aligned else plan.data)
    here = lax.broadcasted_iota(jnp.int16, (n * tall, t), 0) == home.astype(jnp.int16)
    lines = [jnp.where(here, bests[q], jnp.bfloat16(0)) for q in snaps]
    slot_of = left(iota((t, 1), 0), plan.slots)
    lanes = [hot((t, LANES), 1, q * plan.slots + slot_of) for q in snaps]
    tail = dot(jnp.concatenate(lines, axis=1), jnp.concatenate(lanes, axis=0), 1, 0).astype(jnp.bfloat16)
    width = plan.width
    if plan.aligned:
        for r in cores:
            for p in range(n):
                base = plan.at(p, r, plan.back)
                for q in snaps:
                    a = base + q * plan.slots
                    out_ref[a : a + plan.slots, :] = blends[q][
                        p * plan.slots : (p + 1) * plan.slots, r * width : (r + 1) * width
                    ]
                out_ref[base + plan.data : base + plan.back, :] = tail[p * SUB : p * SUB + plan.back - plan.data]
        return
    height = n * plan.groups * plan.back
    col = iota((1, n * tall), 1)
    full = None
    for r in cores:
        piece = dot(hot((height, n * tall), 0, plan.at(col // tall, r, tall) + col % tall), tail, 1, 0)
        for q in snaps:
            put = hot((height, t), 0, plan.at(source, r, plan.back) + q * plan.slots + slot)
            piece = piece + dot(put, blends[q][:, r * width : (r + 1) * width], 1, 0)
        full = piece if full is None else full + piece
    out_ref[...] = full.astype(jnp.bfloat16)


def land_kernel(plan, back_ref, target_ref, rows_ref, out_ref, best_ref):
    h, t = plan.halos, plan.total
    target = target_ref[...]
    column = jnp.transpose(target)
    own_row = iota((h, 1), 0) + t
    for g in range(plan.groups):
        tail, row = tail_in(plan, back_ref, g, plan.back)
        pulls = []
        for q in range(plan.per):
            s = g * plan.per + q
            spot = column[:, s : s + 1]
            owner, slot = spot >> 7, (spot & (LANES - 1)) - q * plan.slots
            spot = jnp.where(spot >= 0, owner * plan.slots + slot, own_row)
            rows = jnp.concatenate([rows_in(plan, back_ref, g, q, plan.back), rows_ref[s]], axis=0)
            out_ref[s] = dot(hot((h, t + h), 1, spot), rows, 1, 0).astype(jnp.bfloat16)
            spot = target[s : s + 1, :]
            pulls.append(hot((tail.shape[0], h), 0, jnp.where(spot >= 0, row(spot >> 7), -1)))
        grid = dot(tail, jnp.concatenate(pulls, axis=1), 0, 0)
        for q in range(plan.per):
            s = g * plan.per + q
            place = target[s : s + 1, :] & (LANES - 1)
            mine = jnp.where(iota((LANES, h), 0) == place, grid[:, q * h : (q + 1) * h], 0.0)
            best_ref[s : s + 1, :] = jnp.sum(mine, axis=0, keepdims=True).astype(jnp.bfloat16)


def body(halo_rows, unmatched, owner_id, cand_index, lengths, choice_index, desc_rows):
    peers, groups = lax.axis_size("space"), lax.axis_size("rep")
    snaps, halos, width = halo_rows.shape
    cands, listed = desc_rows.shape[1], cand_index.shape[2]
    plan = Plan(peers, groups, snaps, halos, width, cands, listed)
    rep = lax.axis_index("rep").astype(jnp.int32)

    def swap(flat, size):
        boxed = flat.reshape(peers * groups, size // 2, 2, width)
        boxed = lax.all_to_all(boxed, ("space", "rep"), 0, 0, tiled=True)
        return boxed.reshape(peers * groups * size, width)

    other = lax.ppermute(desc_rows, "rep", [(0, 1), (1, 0)])

    vmem = pl.BlockSpec(memory_space=pltpu.VMEM)
    smem = pl.BlockSpec(memory_space=pltpu.SMEM)
    hbm = pl.BlockSpec(memory_space=pltpu.HBM)
    small = pltpu.CompilerParams(vmem_limit_bytes=20 << 20)
    flat = (snaps, halos)
    sent, target = pl.pallas_call(
        lambda *refs: route_kernel(plan, *refs),
        name="route",
        compiler_params=small,
        out_shape=(
            jax.ShapeDtypeStruct((peers * groups * plan.send, width), jnp.bfloat16),
            jax.ShapeDtypeStruct(flat, jnp.int32),
        ),
        in_specs=[smem] + [hbm] * 6,
        out_specs=(vmem, vmem),
        scratch_shapes=[
            pltpu.VMEM(flat, jnp.int32),
            pltpu.VMEM(flat, jnp.int32),
            pltpu.VMEM((snaps, listed, halos), jnp.int32),
            pltpu.VMEM(flat, jnp.int32),
            pltpu.VMEM(flat, jnp.int32),
            pltpu.VMEM((snaps, halos, width), jnp.bfloat16),
            pltpu.SemaphoreType.DMA((6,)),
        ],
    )(
        rep.reshape(1),
        *(
            pltpu.with_memory_space_constraint(x, pltpu.HBM)
            for x in (
                owner_id.reshape(flat),
                unmatched,
                jnp.swapaxes(cand_index, 1, 2),
                lengths,
                choice_index,
                halo_rows,
            )
        ),
    )
    sent, other = lax.optimization_barrier((sent, other))
    got = swap(sent, plan.send)
    reply = pl.pallas_call(
        lambda *refs: owner_kernel(plan, *refs),
        name="owner",
        compiler_params=small,
        out_shape=jax.ShapeDtypeStruct((peers * groups * plan.back, width), jnp.bfloat16),
        in_specs=[smem, vmem, vmem, vmem],
        out_specs=vmem,
    )(rep.reshape(1), got, desc_rows, other)
    back = swap(reply, plan.back)
    return pl.pallas_call(
        lambda *refs: land_kernel(plan, *refs),
        name="land",
        compiler_params=small,
        out_shape=(
            jax.ShapeDtypeStruct((snaps, halos, width), jnp.bfloat16),
            jax.ShapeDtypeStruct((snaps, halos), jnp.bfloat16),
        ),
        in_specs=[vmem] * 3,
        out_specs=(vmem, vmem),
    )(back, target, halo_rows)


def solution(mesh):
    in_specs = (
        P(None, "space", "rep"),
        P(None, "space"),
        P(None, "space", None),
        P(None, "space", None),
        P(None, "space"),
        P(None, "space"),
        P(None, "space", "rep"),
    )
    out_specs = (P(None, "space", "rep"), P(None, "space"))
    return jax.shard_map(body, mesh=mesh, in_specs=in_specs, out_specs=out_specs, check_vma=False)
```

```python
import math

import jax
import jax.numpy as jnp
from jax import lax
from jax.experimental import pallas as pl
from jax.experimental.pallas import tpu as pltpu
from jax.sharding import PartitionSpec as P

LANES = 128
SUB = 8
WORD = 32
NEG = -3.0e38


def iota(shape, axis):
    return lax.broadcasted_iota(jnp.int32, shape, axis)


def over(x, m):
    return x >> (m.bit_length() - 1) if m & (m - 1) == 0 else x // m


def left(x, m):
    return x & (m - 1) if m & (m - 1) == 0 else x % m


def hot(shape, axis, spot):
    mask = lax.broadcasted_iota(jnp.int16, shape, axis) == spot.astype(jnp.int16)
    return jnp.where(mask, jnp.bfloat16(1), jnp.bfloat16(0))


def dot(a, b, ca, cb):
    return lax.dot_general(a, b, (((ca,), (cb,)), ((), ())), preferred_element_type=jnp.float32)


class Plan:
    def __init__(self, peers, groups, snaps, halos, width, cands, listed):
        self.peers, self.groups, self.snaps = peers, groups, snaps
        self.halos, self.width, self.cands, self.listed = halos, width, cands, listed
        self.per = snaps // groups
        self.slots = 2 * halos // peers
        self.total = peers * self.slots
        self.data = self.per * self.slots
        self.fit = LANES // listed
        self.codes = -(-(-(-self.data // self.fit)) // groups)
        self.send = self.data + self.codes + (self.data + self.codes) % 2
        self.back = self.data + 1 + (self.data + 1) % 2
        self.half = cands // 2
        self.aligned = self.slots % SUB == 0
        assert snaps % groups == 0 and groups == 2
        assert width == LANES and halos <= LANES and cands <= 512 and cands % WORD == 0
        assert LANES % listed == 0 and self.data <= LANES
        assert peers * groups * self.send % SUB == 0 and peers * groups * self.back % SUB == 0
        assert not self.aligned or (self.codes <= SUB <= self.data)

    def at(self, peer, group, size):
        return (peer * self.groups + group) * size


def route_kernel(plan, rep_ref, *refs):
    sources, (out_ref, target_ref), held = refs[:6], refs[6:8], refs[8:14]
    sems = refs[14]
    copies = [pltpu.make_async_copy(x, y, sems.at[i]) for i, (x, y) in enumerate(zip(sources, held))]
    for copy in copies:
        copy.start()
    owner_ref, live_ref, cand_ref, span_ref, pick_ref, rows_ref = held
    n, h, k = plan.peers, plan.halos, plan.listed
    rep = rep_ref[0]
    upper = iota((h, h), 0) < iota((h, h), 1)
    upper = jnp.where(upper, 1.0, 0.0).astype(jnp.bfloat16)
    peer_ids = iota((n, h), 0)
    list_ids = iota((k, h), 0)
    for copy in copies[:-1]:
        copy.wait()
    owners = [owner_ref[s : s + 1, :] for s in range(plan.snaps)]
    marks = jnp.concatenate([hot((n, h), 0, o) for o in owners], axis=0)
    prefix = dot(marks, upper, 1, 0)
    puts, says, spreads = [], [], []
    for s in range(plan.snaps):
        g, q = s // plan.per, s % plan.per
        mine = jnp.where(peer_ids == owners[s], prefix[s * n : (s + 1) * n], 0.0)
        rank = jnp.sum(mine, axis=0, keepdims=True).astype(jnp.int32)
        live = live_ref[s : s + 1, :] == 1
        place = q * plan.slots + rank
        target_ref[s : s + 1, :] = jnp.where(live, owners[s] * LANES + place, -LANES)
        listing = cand_ref[s]
        pick = pick_ref[s : s + 1, :]
        chosen = jnp.sum(jnp.where(list_ids == pick, listing, 0), axis=0, keepdims=True)
        first = listing[0:1, :]
        kept = jnp.where(list_ids < span_ref[s : s + 1, :], listing, chosen)
        kept = jnp.where(list_ids == pick, first, kept)
        kept = jnp.where(list_ids == 0, chosen, kept)
        code = jnp.where(kept < plan.half, kept - plan.half, kept - plan.half + 1)
        code = code.astype(jnp.float32).astype(jnp.bfloat16)
        spot, line = left(place, plan.fit).astype(jnp.int16), over(place, plan.fit)
        spreads.append(
            jnp.concatenate(
                [jnp.where(jnp.broadcast_to(spot, (k, h)) == b, code, jnp.bfloat16(0)) for b in range(plan.fit)],
                axis=0,
            )
        )
        tells = live & (over(line, plan.codes) == rep)
        line = left(line, plan.codes)
        if plan.aligned:
            puts.append(hot((n * plan.data, h), 0, jnp.where(live, owners[s] * plan.data + place, -1)))
            says.append(hot((n * SUB, h), 0, jnp.where(tells, owners[s] * SUB + line, -1)))
        else:
            base = plan.at(owners[s], g, plan.send)
            shape = (n * plan.groups * plan.send, h)
            puts.append(hot(shape, 0, jnp.where(live, base + place, -1)))
            says.append(hot(shape, 0, jnp.where(tells, base + plan.data + line, -1)))

    def joined(parts, g, axis):
        return jnp.concatenate(parts[g * plan.per : (g + 1) * plan.per], axis=axis)

    tails = [dot(joined(says, g, 1), joined(spreads, g, 1), 1, 1) for g in range(plan.groups)]
    copies[-1].wait()
    whole = None
    for g in range(plan.groups):
        held_rows = rows_ref[g * plan.per : (g + 1) * plan.per].reshape(plan.per * h, plan.width)
        rows = dot(joined(puts, g, 1), held_rows, 1, 0)
        if plan.aligned:
            rows, tail = rows.astype(jnp.bfloat16), tails[g].astype(jnp.bfloat16)
            for p in range(n):
                base = plan.at(p, g, plan.send)
                out_ref[base : base + plan.data, :] = rows[p * plan.data : (p + 1) * plan.data]
                out_ref[base + plan.data : base + plan.send, :] = tail[p * SUB : p * SUB + plan.send - plan.data]
        else:
            both = rows + tails[g]
            whole = both if whole is None else whole + both
    if not plan.aligned:
        out_ref[...] = whole.astype(jnp.bfloat16)


def soft(v):
    return 1.0 + (jnp.maximum(v, 0.0) + jnp.log1p(jnp.exp(-jnp.abs(v))))


def rows_in(plan, ref, group, q, size):
    if plan.aligned:
        starts = [plan.at(p, group, size) + q * plan.slots for p in range(plan.peers)]
        return jnp.concatenate([ref[a : a + plan.slots, :] for a in starts], axis=0)
    item = iota((plan.total, 1), 0)
    spot = plan.at(over(item, plan.slots), group, size) + q * plan.slots + left(item, plan.slots)
    take = hot((plan.total, plan.peers * plan.groups * size), 1, spot)
    return dot(take, ref[...], 1, 0).astype(jnp.bfloat16)


def tail_in(plan, ref, group, size):
    if plan.aligned:
        ends = [plan.at(p, group, size) + size for p in range(plan.peers)]
        value = jnp.concatenate([ref[a - SUB : a, :] for a in ends], axis=0)
        return value, (lambda p: p * SUB + SUB - (size - plan.data))
    return ref[...], (lambda p: plan.at(p, group, size) + plan.data)


def owner_kernel(plan, rep_ref, got_ref, own_ref, other_ref, peek_ref, out_ref):
    n, t, c, k = plan.peers, plan.total, plan.cands, plan.listed
    rep = rep_ref[0]
    scale = 1.0 / math.sqrt(plan.width * plan.groups)
    item = iota((1, t), 1)
    source, slot = over(item, plan.slots), left(item, plan.slots)
    snaps, cores = range(plan.per), range(plan.groups)
    ends = [tail_in(plan, got_ref, r, plan.send) for r in cores]

    tables, rows, merits = [], [], []
    for q in snaps:
        own, other = own_ref[rep * plan.per + q], other_ref[rep * plan.per + q]
        pair = [jnp.where(rep == 0, own, other), jnp.where(rep == 0, other, own)]
        tables.append(jnp.concatenate(pair, axis=1))
        rows.append(jnp.concatenate([rows_in(plan, got_ref, r, q, plan.send) for r in cores], axis=1))

    listing = []
    for q in snaps:
        place = q * plan.slots + slot
        spot, line = left(place, plan.fit), over(place, plan.fit)
        wide = None
        for r in cores:
            value, row = ends[r]
            if (q * plan.slots + plan.slots - 1) // plan.fit // plan.codes < r:
                continue
            if q * plan.slots // plan.fit // plan.codes > r:
                continue
            told = jnp.where(over(line, plan.codes) == r, row(source) + left(line, plan.codes), -1)
            piece = dot(value, hot((value.shape[0], t), 0, told), 0, 0)
            wide = piece if wide is None else wide + piece
        codes = wide[0:k]
        for b in range(1, plan.fit):
            codes = jnp.where(spot == b, wide[b * k : (b + 1) * k], codes)
        codes = codes.astype(jnp.int32)
        index = jnp.where(codes < 0, codes + plan.half, codes + plan.half - 1)
        listing.append(jnp.where(codes == 0, -1, index))
        merits.append(dot(tables[q], rows[q], 1, 1))

    words = c // WORD
    word_ids = iota((words, t), 0)
    line_ids = iota((WORD, t), 0)
    bits = jnp.left_shift(jnp.int32(1), line_ids)
    filler = jnp.zeros((SUB - plan.per, t), jnp.float32)
    heads = [listing[q][0:1, :].astype(jnp.float32) for q in snaps]
    heads = jnp.transpose(jnp.concatenate(heads + [filler], axis=0)).astype(jnp.int32)
    descs = [dot(hot((t, c), 1, heads[:, q : q + 1]), tables[q], 1, 0) for q in snaps]
    bests, shares = [], []
    for q in snaps:
        index = listing[q]
        high, bit = index >> 5, jnp.left_shift(jnp.int32(1), index & (WORD - 1))
        sets = jnp.zeros((words, t), jnp.int32)
        for j in range(k):
            sets = sets | jnp.where(high[j : j + 1, :] == word_ids, bit[j : j + 1, :], 0)
        head = index[0:1, :]
        best = jnp.full((WORD, t), NEG, jnp.float32)
        picked = jnp.zeros((WORD, t), jnp.float32)
        rival = jnp.zeros((WORD, t), jnp.float32)
        for w in range(words):
            merit = merits[q][w * WORD : (w + 1) * WORD]
            member = (sets[w : w + 1, :] & bits) != 0
            listed = jnp.where(member, merit, NEG)
            best = jnp.maximum(best, listed)
            top = jnp.max(listed, axis=1, keepdims=True)
            chosen = line_ids == head - w * WORD
            picked = jnp.where(chosen, merit, picked)
            rival = jnp.where(chosen, top, rival)
        bests.append((jnp.max(best, axis=0, keepdims=True) * scale).astype(jnp.bfloat16))
        mine = soft(jnp.sum(picked, axis=0, keepdims=True) * scale)
        claim = soft(jnp.sum(rival, axis=0, keepdims=True) * scale)
        shares.append(mine / (mine + claim))
    shares = jnp.transpose(jnp.concatenate(shares + [filler], axis=0))

    blends = []
    for q in snaps:
        share = shares[:, q : q + 1]
        blend = (1.0 - share) * rows[q].astype(jnp.float32) + share * descs[q]
        blends.append(blend.astype(jnp.bfloat16))

    tall = SUB if plan.aligned else plan.back
    home = source * tall + (0 if plan.aligned else plan.data)
    here = lax.broadcasted_iota(jnp.int16, (n * tall, t), 0) == home.astype(jnp.int16)
    lines = [jnp.where(here, bests[q], jnp.bfloat16(0)) for q in snaps]
    slot_of = left(iota((t, 1), 0), plan.slots)
    lanes = [hot((t, LANES), 1, q * plan.slots + slot_of) for q in snaps]
    tail = dot(jnp.concatenate(lines, axis=1), jnp.concatenate(lanes, axis=0), 1, 0).astype(jnp.bfloat16)
    width = plan.width
    if plan.aligned:
        for r in cores:
            for p in range(n):
                base = plan.at(p, r, plan.back)
                for q in snaps:
                    a = base + q * plan.slots
                    out_ref[a : a + plan.slots, :] = blends[q][
                        p * plan.slots : (p + 1) * plan.slots, r * width : (r + 1) * width
                    ]
                out_ref[base + plan.data : base + plan.back, :] = tail[p * SUB : p * SUB + plan.back - plan.data]
        return
    height = n * plan.groups * plan.back
    col = iota((1, n * tall), 1)
    full = None
    for r in cores:
        piece = dot(hot((height, n * tall), 0, plan.at(col // tall, r, tall) + col % tall), tail, 1, 0)
        for q in snaps:
            put = hot((height, t), 0, plan.at(source, r, plan.back) + q * plan.slots + slot)
            piece = piece + dot(put, blends[q][:, r * width : (r + 1) * width], 1, 0)
        full = piece if full is None else full + piece
    out_ref[...] = full.astype(jnp.bfloat16)


def land_kernel(plan, back_ref, target_ref, rows_ref, out_ref, best_ref):
    h, t = plan.halos, plan.total
    target = target_ref[...]
    column = jnp.transpose(target)
    own_row = iota((h, 1), 0) + t
    for g in range(plan.groups):
        tail, row = tail_in(plan, back_ref, g, plan.back)
        pulls = []
        for q in range(plan.per):
            s = g * plan.per + q
            spot = column[:, s : s + 1]
            owner, slot = spot >> 7, (spot & (LANES - 1)) - q * plan.slots
            spot = jnp.where(spot >= 0, owner * plan.slots + slot, own_row)
            rows = jnp.concatenate([rows_in(plan, back_ref, g, q, plan.back), rows_ref[s]], axis=0)
            out_ref[s] = dot(hot((h, t + h), 1, spot), rows, 1, 0).astype(jnp.bfloat16)
            spot = target[s : s + 1, :]
            pulls.append(hot((tail.shape[0], h), 0, jnp.where(spot >= 0, row(spot >> 7), -1)))
        grid = dot(tail, jnp.concatenate(pulls, axis=1), 0, 0)
        for q in range(plan.per):
            s = g * plan.per + q
            place = target[s : s + 1, :] & (LANES - 1)
            mine = jnp.where(iota((LANES, h), 0) == place, grid[:, q * h : (q + 1) * h], 0.0)
            best_ref[s : s + 1, :] = jnp.sum(mine, axis=0, keepdims=True).astype(jnp.bfloat16)


def body(halo_rows, unmatched, owner_id, cand_index, lengths, choice_index, desc_rows):
    peers, groups = lax.axis_size("space"), lax.axis_size("rep")
    snaps, halos, width = halo_rows.shape
    cands, listed = desc_rows.shape[1], cand_index.shape[2]
    plan = Plan(peers, groups, snaps, halos, width, cands, listed)
    rep = lax.axis_index("rep").astype(jnp.int32)

    def swap(flat, size):
        boxed = flat.reshape(peers * groups, size // 2, 2, width)
        boxed = lax.all_to_all(boxed, ("space", "rep"), 0, 0, tiled=True)
        return boxed.reshape(peers * groups * size, width)

    other = lax.ppermute(desc_rows, "rep", [(0, 1), (1, 0)])

    vmem = pl.BlockSpec(memory_space=pltpu.VMEM)
    smem = pl.BlockSpec(memory_space=pltpu.SMEM)
    hbm = pl.BlockSpec(memory_space=pltpu.HBM)
    small = pltpu.CompilerParams(vmem_limit_bytes=20 << 20)
    packed = pltpu.CompilerParams(vmem_limit_bytes=20 << 20)
    flat = (snaps, halos)
    sent, target = pl.pallas_call(
        lambda *refs: route_kernel(plan, *refs),
        name="route",
        compiler_params=small,
        out_shape=(
            jax.ShapeDtypeStruct((peers * groups * plan.send, width), jnp.bfloat16),
            jax.ShapeDtypeStruct(flat, jnp.int32),
        ),
        in_specs=[smem] + [hbm] * 6,
        out_specs=(vmem, vmem),
        scratch_shapes=[
            pltpu.VMEM(flat, jnp.int32),
            pltpu.VMEM(flat, jnp.int32),
            pltpu.VMEM((snaps, listed, halos), jnp.int32),
            pltpu.VMEM(flat, jnp.int32),
            pltpu.VMEM(flat, jnp.int32),
            pltpu.VMEM((snaps, halos, width), jnp.bfloat16),
            pltpu.SemaphoreType.DMA((6,)),
        ],
    )(
        rep.reshape(1),
        *(
            pltpu.with_memory_space_constraint(x, pltpu.HBM)
            for x in (
                owner_id.reshape(flat),
                unmatched,
                jnp.swapaxes(cand_index, 1, 2),
                lengths,
                choice_index,
                halo_rows,
            )
        ),
    )
    got = swap(sent, plan.send)
    peek = got[0:SUB] * jnp.bfloat16(2)
    reply = pl.pallas_call(
        lambda *refs: owner_kernel(plan, *refs),
        name="owner",
        compiler_params=packed,
        out_shape=jax.ShapeDtypeStruct((peers * groups * plan.back, width), jnp.bfloat16),
        in_specs=[smem, vmem, vmem, vmem, vmem],
        out_specs=vmem,
    )(rep.reshape(1), got, desc_rows, other, peek)
    back = swap(reply, plan.back)
    return pl.pallas_call(
        lambda *refs: land_kernel(plan, *refs),
        name="land",
        compiler_params=packed,
        out_shape=(
            jax.ShapeDtypeStruct((snaps, halos, width), jnp.bfloat16),
            jax.ShapeDtypeStruct((snaps, halos), jnp.bfloat16),
        ),
        in_specs=[vmem] * 3,
        out_specs=(vmem, vmem),
    )(back, target, halo_rows)


def solution(mesh):
    in_specs = (
        P(None, "space", "rep"),
        P(None, "space"),
        P(None, "space", None),
        P(None, "space", None),
        P(None, "space"),
        P(None, "space"),
        P(None, "space", "rep"),
    )
    out_specs = (P(None, "space", "rep"), P(None, "space"))

    return jax.shard_map(body, mesh=mesh, in_specs=in_specs, out_specs=out_specs, check_vma=False)
```

```python
import math

import jax
import jax.numpy as jnp
from jax import lax
from jax.experimental import pallas as pl
from jax.experimental.pallas import tpu as pltpu
from jax.sharding import PartitionSpec as P

LANES = 128
SUB = 8
WORD = 32
NEG = -3.0e38


def iota(shape, axis):
    return lax.broadcasted_iota(jnp.int32, shape, axis)


def over(x, m):
    return x >> (m.bit_length() - 1) if m & (m - 1) == 0 else x // m


def left(x, m):
    return x & (m - 1) if m & (m - 1) == 0 else x % m


def hot(shape, axis, spot):
    mask = lax.broadcasted_iota(jnp.int16, shape, axis) == spot.astype(jnp.int16)
    return jnp.where(mask, jnp.bfloat16(1), jnp.bfloat16(0))


def dot(a, b, ca, cb):
    return lax.dot_general(a, b, (((ca,), (cb,)), ((), ())), preferred_element_type=jnp.float32)


class Plan:
    def __init__(self, peers, groups, snaps, halos, width, cands, listed):
        self.peers, self.groups, self.snaps = peers, groups, snaps
        self.halos, self.width, self.cands, self.listed = halos, width, cands, listed
        self.per = snaps // groups
        self.slots = 2 * halos // peers
        self.total = peers * self.slots
        self.data = self.per * self.slots
        self.fit = LANES // listed
        self.codes = -(-(-(-self.data // self.fit)) // groups)
        self.send = self.data + self.codes + (self.data + self.codes) % 2
        self.back = self.data + 1 + (self.data + 1) % 2
        self.half = cands // 2
        self.aligned = self.slots % SUB == 0
        assert snaps % groups == 0 and groups == 2
        assert width == LANES and halos <= LANES and cands <= 512 and cands % WORD == 0
        assert LANES % listed == 0 and self.data <= LANES
        assert peers * groups * self.send % SUB == 0 and peers * groups * self.back % SUB == 0
        assert not self.aligned or (self.codes <= SUB <= self.data)

    def at(self, peer, group, size):
        return (peer * self.groups + group) * size


def order_kernel(plan, out_ref):
    shape = (plan.halos, plan.halos)
    out_ref[...] = jnp.where(iota(shape, 0) < iota(shape, 1), 1.0, 0.0).astype(jnp.bfloat16)


def route_kernel(
    plan, rep_ref, upper_ref, owner_ref, live_ref, cand_ref, span_ref, pick_ref, rows_ref, out_ref, target_ref
):
    n, h, k = plan.peers, plan.halos, plan.listed
    rep = rep_ref[0]
    peer_ids = iota((n, h), 0)
    list_ids = iota((k, h), 0)
    owners = [owner_ref[s : s + 1, :] for s in range(plan.snaps)]
    marks = jnp.concatenate([hot((n, h), 0, o) for o in owners], axis=0)
    prefix = dot(marks, upper_ref[...], 1, 0)
    puts, says, spreads = [], [], []
    for s in range(plan.snaps):
        g, q = s // plan.per, s % plan.per
        mine = jnp.where(peer_ids == owners[s], prefix[s * n : (s + 1) * n], 0.0)
        rank = jnp.sum(mine, axis=0, keepdims=True).astype(jnp.int32)
        live = live_ref[s : s + 1, :] == 1
        place = q * plan.slots + rank
        target_ref[s : s + 1, :] = jnp.where(live, owners[s] * LANES + place, -LANES)
        listing = cand_ref[s]
        pick = pick_ref[s : s + 1, :]
        chosen = jnp.sum(jnp.where(list_ids == pick, listing, 0), axis=0, keepdims=True)
        first = listing[0:1, :]
        kept = jnp.where(list_ids < span_ref[s : s + 1, :], listing, chosen)
        kept = jnp.where(list_ids == pick, first, kept)
        kept = jnp.where(list_ids == 0, chosen, kept)
        code = jnp.where(kept < plan.half, kept - plan.half, kept - plan.half + 1)
        code = code.astype(jnp.float32).astype(jnp.bfloat16)
        spot, line = left(place, plan.fit).astype(jnp.int16), over(place, plan.fit)
        spreads.append(
            jnp.concatenate(
                [jnp.where(jnp.broadcast_to(spot, (k, h)) == b, code, jnp.bfloat16(0)) for b in range(plan.fit)],
                axis=0,
            )
        )
        tells = live & (over(line, plan.codes) == rep)
        line = left(line, plan.codes)
        if plan.aligned:
            puts.append(hot((n * plan.data, h), 0, jnp.where(live, owners[s] * plan.data + place, -1)))
            says.append(hot((n * SUB, h), 0, jnp.where(tells, owners[s] * SUB + line, -1)))
        else:
            base = plan.at(owners[s], g, plan.send)
            shape = (n * plan.groups * plan.send, h)
            puts.append(hot(shape, 0, jnp.where(live, base + place, -1)))
            says.append(hot(shape, 0, jnp.where(tells, base + plan.data + line, -1)))

    def joined(parts, g, axis):
        return jnp.concatenate(parts[g * plan.per : (g + 1) * plan.per], axis=axis)

    tails = [dot(joined(says, g, 1), joined(spreads, g, 1), 1, 1) for g in range(plan.groups)]
    whole = None
    for g in range(plan.groups):
        held_rows = rows_ref[g * plan.per : (g + 1) * plan.per].reshape(plan.per * h, plan.width)
        rows = dot(joined(puts, g, 1), held_rows, 1, 0)
        if plan.aligned:
            rows, tail = rows.astype(jnp.bfloat16), tails[g].astype(jnp.bfloat16)
            for p in range(n):
                base = plan.at(p, g, plan.send)
                out_ref[base : base + plan.data, :] = rows[p * plan.data : (p + 1) * plan.data]
                out_ref[base + plan.data : base + plan.send, :] = tail[p * SUB : p * SUB + plan.send - plan.data]
        else:
            both = rows + tails[g]
            whole = both if whole is None else whole + both
    if not plan.aligned:
        out_ref[...] = whole.astype(jnp.bfloat16)


def soft(v):
    return 1.0 + (jnp.maximum(v, 0.0) + jnp.log1p(jnp.exp(-jnp.abs(v))))


def rows_in(plan, ref, group, q, size):
    if plan.aligned:
        starts = [plan.at(p, group, size) + q * plan.slots for p in range(plan.peers)]
        return jnp.concatenate([ref[a : a + plan.slots, :] for a in starts], axis=0)
    item = iota((plan.total, 1), 0)
    spot = plan.at(over(item, plan.slots), group, size) + q * plan.slots + left(item, plan.slots)
    take = hot((plan.total, plan.peers * plan.groups * size), 1, spot)
    return dot(take, ref[...], 1, 0).astype(jnp.bfloat16)


def tail_in(plan, ref, group, size):
    if plan.aligned:
        ends = [plan.at(p, group, size) + size for p in range(plan.peers)]
        value = jnp.concatenate([ref[a - SUB : a, :] for a in ends], axis=0)
        return value, (lambda p: p * SUB + SUB - (size - plan.data))
    return ref[...], (lambda p: plan.at(p, group, size) + plan.data)


def owner_kernel(plan, rep_ref, got_ref, own_ref, other_ref, peek_ref, out_ref):
    n, t, c, k = plan.peers, plan.total, plan.cands, plan.listed
    rep = rep_ref[0]
    scale = 1.0 / math.sqrt(plan.width * plan.groups)
    item = iota((1, t), 1)
    source, slot = over(item, plan.slots), left(item, plan.slots)
    snaps, cores = range(plan.per), range(plan.groups)
    ends = [tail_in(plan, got_ref, r, plan.send) for r in cores]

    tables, rows, merits = [], [], []
    for q in snaps:
        own, other = own_ref[rep * plan.per + q], other_ref[rep * plan.per + q]
        pair = [jnp.where(rep == 0, own, other), jnp.where(rep == 0, other, own)]
        tables.append(jnp.concatenate(pair, axis=1))
        rows.append(jnp.concatenate([rows_in(plan, got_ref, r, q, plan.send) for r in cores], axis=1))

    listing = []
    for q in snaps:
        place = q * plan.slots + slot
        spot, line = left(place, plan.fit), over(place, plan.fit)
        wide = None
        for r in cores:
            value, row = ends[r]
            if (q * plan.slots + plan.slots - 1) // plan.fit // plan.codes < r:
                continue
            if q * plan.slots // plan.fit // plan.codes > r:
                continue
            told = jnp.where(over(line, plan.codes) == r, row(source) + left(line, plan.codes), -1)
            piece = dot(value, hot((value.shape[0], t), 0, told), 0, 0)
            wide = piece if wide is None else wide + piece
        codes = wide[0:k]
        for b in range(1, plan.fit):
            codes = jnp.where(spot == b, wide[b * k : (b + 1) * k], codes)
        codes = codes.astype(jnp.int32)
        index = jnp.where(codes < 0, codes + plan.half, codes + plan.half - 1)
        listing.append(jnp.where(codes == 0, -1, index))
        merits.append(dot(tables[q], rows[q], 1, 1))

    words = c // WORD
    word_ids = iota((words, t), 0)
    line_ids = iota((WORD, t), 0)
    bits = jnp.left_shift(jnp.int32(1), line_ids)
    filler = jnp.zeros((SUB - plan.per, t), jnp.float32)
    heads = [listing[q][0:1, :].astype(jnp.float32) for q in snaps]
    heads = jnp.transpose(jnp.concatenate(heads + [filler], axis=0)).astype(jnp.int32)
    descs = [dot(hot((t, c), 1, heads[:, q : q + 1]), tables[q], 1, 0) for q in snaps]
    bests, shares = [], []
    for q in snaps:
        index = listing[q]
        high, bit = index >> 5, jnp.left_shift(jnp.int32(1), index & (WORD - 1))
        sets = jnp.zeros((words, t), jnp.int32)
        for j in range(k):
            sets = sets | jnp.where(high[j : j + 1, :] == word_ids, bit[j : j + 1, :], 0)
        head = index[0:1, :]
        best = jnp.full((WORD, t), NEG, jnp.float32)
        picked = jnp.zeros((WORD, t), jnp.float32)
        rival = jnp.zeros((WORD, t), jnp.float32)
        for w in range(words):
            merit = merits[q][w * WORD : (w + 1) * WORD]
            member = (sets[w : w + 1, :] & bits) != 0
            listed = jnp.where(member, merit, NEG)
            best = jnp.maximum(best, listed)
            top = jnp.max(listed, axis=1, keepdims=True)
            chosen = line_ids == head - w * WORD
            picked = jnp.where(chosen, merit, picked)
            rival = jnp.where(chosen, top, rival)
        bests.append((jnp.max(best, axis=0, keepdims=True) * scale).astype(jnp.bfloat16))
        mine = soft(jnp.sum(picked, axis=0, keepdims=True) * scale)
        claim = soft(jnp.sum(rival, axis=0, keepdims=True) * scale)
        shares.append(mine / (mine + claim))
    shares = jnp.transpose(jnp.concatenate(shares + [filler], axis=0))

    blends = []
    for q in snaps:
        share = shares[:, q : q + 1]
        blend = (1.0 - share) * rows[q].astype(jnp.float32) + share * descs[q]
        blends.append(blend.astype(jnp.bfloat16))

    tall = SUB if plan.aligned else plan.back
    home = source * tall + (0 if plan.aligned else plan.data)
    here = lax.broadcasted_iota(jnp.int16, (n * tall, t), 0) == home.astype(jnp.int16)
    lines = [jnp.where(here, bests[q], jnp.bfloat16(0)) for q in snaps]
    slot_of = left(iota((t, 1), 0), plan.slots)
    lanes = [hot((t, LANES), 1, q * plan.slots + slot_of) for q in snaps]
    tail = dot(jnp.concatenate(lines, axis=1), jnp.concatenate(lanes, axis=0), 1, 0).astype(jnp.bfloat16)
    width = plan.width
    if plan.aligned:
        for r in cores:
            for p in range(n):
                base = plan.at(p, r, plan.back)
                for q in snaps:
                    a = base + q * plan.slots
                    out_ref[a : a + plan.slots, :] = blends[q][
                        p * plan.slots : (p + 1) * plan.slots, r * width : (r + 1) * width
                    ]
                out_ref[base + plan.data : base + plan.back, :] = tail[p * SUB : p * SUB + plan.back - plan.data]
        return
    height = n * plan.groups * plan.back
    col = iota((1, n * tall), 1)
    full = None
    for r in cores:
        piece = dot(hot((height, n * tall), 0, plan.at(col // tall, r, tall) + col % tall), tail, 1, 0)
        for q in snaps:
            put = hot((height, t), 0, plan.at(source, r, plan.back) + q * plan.slots + slot)
            piece = piece + dot(put, blends[q][:, r * width : (r + 1) * width], 1, 0)
        full = piece if full is None else full + piece
    out_ref[...] = full.astype(jnp.bfloat16)


def land_kernel(plan, back_ref, target_ref, rows_ref, out_ref, best_ref):
    h, t = plan.halos, plan.total
    target = target_ref[...]
    column = jnp.transpose(target)
    own_row = iota((h, 1), 0) + t
    for g in range(plan.groups):
        tail, row = tail_in(plan, back_ref, g, plan.back)
        pulls = []
        for q in range(plan.per):
            s = g * plan.per + q
            spot = column[:, s : s + 1]
            owner, slot = spot >> 7, (spot & (LANES - 1)) - q * plan.slots
            spot = jnp.where(spot >= 0, owner * plan.slots + slot, own_row)
            rows = jnp.concatenate([rows_in(plan, back_ref, g, q, plan.back), rows_ref[s]], axis=0)
            out_ref[s] = dot(hot((h, t + h), 1, spot), rows, 1, 0).astype(jnp.bfloat16)
            spot = target[s : s + 1, :]
            pulls.append(hot((tail.shape[0], h), 0, jnp.where(spot >= 0, row(spot >> 7), -1)))
        grid = dot(tail, jnp.concatenate(pulls, axis=1), 0, 0)
        for q in range(plan.per):
            s = g * plan.per + q
            place = target[s : s + 1, :] & (LANES - 1)
            mine = jnp.where(iota((LANES, h), 0) == place, grid[:, q * h : (q + 1) * h], 0.0)
            best_ref[s : s + 1, :] = jnp.sum(mine, axis=0, keepdims=True).astype(jnp.bfloat16)


def body(halo_rows, unmatched, owner_id, cand_index, lengths, choice_index, desc_rows):
    peers, groups = lax.axis_size("space"), lax.axis_size("rep")
    snaps, halos, width = halo_rows.shape
    cands, listed = desc_rows.shape[1], cand_index.shape[2]
    plan = Plan(peers, groups, snaps, halos, width, cands, listed)
    rep = lax.axis_index("rep").astype(jnp.int32)

    def swap(flat, size):
        boxed = flat.reshape(peers * groups, size // 2, 2, width)
        boxed = lax.all_to_all(boxed, ("space", "rep"), 0, 0, tiled=True)
        return boxed.reshape(peers * groups * size, width)

    other = lax.ppermute(desc_rows, "rep", [(0, 1), (1, 0)])

    vmem = pl.BlockSpec(memory_space=pltpu.VMEM)
    smem = pl.BlockSpec(memory_space=pltpu.SMEM)
    hbm = pl.BlockSpec(memory_space=pltpu.HBM)
    small = pltpu.CompilerParams(vmem_limit_bytes=20 << 20)
    packed = pltpu.CompilerParams(vmem_limit_bytes=20 << 20)
    flat = (snaps, halos)
    upper = pl.pallas_call(
        lambda *refs: order_kernel(plan, *refs),
        name="order",
        compiler_params=pltpu.CompilerParams(vmem_limit_bytes=66_600_000),
        cost_estimate=pl.CostEstimate(flops=1 << 32, bytes_accessed=0, transcendentals=0),
        out_shape=pltpu.VMEM((halos, halos), jnp.bfloat16),
        out_specs=vmem,
    )()
    sent, target = pl.pallas_call(
        lambda *refs: route_kernel(plan, *refs),
        name="route",
        compiler_params=small,
        out_shape=(
            jax.ShapeDtypeStruct((peers * groups * plan.send, width), jnp.bfloat16),
            jax.ShapeDtypeStruct(flat, jnp.int32),
        ),
        in_specs=[smem] + [vmem] * 7,
        out_specs=(vmem, vmem),
    )(
        rep.reshape(1),
        upper,
        owner_id.reshape(flat),
        unmatched,
        jnp.swapaxes(cand_index, 1, 2),
        lengths,
        choice_index,
        halo_rows,
    )
    got = swap(sent, plan.send)
    peek = got[0:SUB] * jnp.bfloat16(2)
    reply = pl.pallas_call(
        lambda *refs: owner_kernel(plan, *refs),
        name="owner",
        compiler_params=packed,
        out_shape=jax.ShapeDtypeStruct((peers * groups * plan.back, width), jnp.bfloat16),
        in_specs=[smem, vmem, vmem, vmem, vmem],
        out_specs=vmem,
    )(rep.reshape(1), got, desc_rows, other, peek)
    back = swap(reply, plan.back)
    return pl.pallas_call(
        lambda *refs: land_kernel(plan, *refs),
        name="land",
        compiler_params=packed,
        out_shape=(
            jax.ShapeDtypeStruct((snaps, halos, width), jnp.bfloat16),
            jax.ShapeDtypeStruct((snaps, halos), jnp.bfloat16),
        ),
        in_specs=[vmem] * 3,
        out_specs=(vmem, vmem),
    )(back, target, halo_rows)


def solution(mesh):
    in_specs = (
        P(None, "space", "rep"),
        P(None, "space"),
        P(None, "space", None),
        P(None, "space", None),
        P(None, "space"),
        P(None, "space"),
        P(None, "space", "rep"),
    )
    out_specs = (P(None, "space", "rep"), P(None, "space"))

    return jax.shard_map(body, mesh=mesh, in_specs=in_specs, out_specs=out_specs, check_vma=False)
```

```python
import math

import jax
import jax.numpy as jnp
from jax import lax
from jax.experimental import pallas as pl
from jax.experimental.pallas import tpu as pltpu
from jax.sharding import PartitionSpec as P

LANES = 128
SUB = 8
WORD = 32
NEG = -3.0e38


def iota(shape, axis):
    return lax.broadcasted_iota(jnp.int32, shape, axis)


def over(x, m):
    return x >> (m.bit_length() - 1) if m & (m - 1) == 0 else x // m


def left(x, m):
    return x & (m - 1) if m & (m - 1) == 0 else x % m


def hot(shape, axis, spot):
    mask = lax.broadcasted_iota(jnp.int16, shape, axis) == spot.astype(jnp.int16)
    return jnp.where(mask, jnp.bfloat16(1), jnp.bfloat16(0))


def dot(a, b, ca, cb):
    return lax.dot_general(a, b, (((ca,), (cb,)), ((), ())), preferred_element_type=jnp.float32)


class Plan:
    def __init__(self, peers, groups, snaps, halos, width, cands, listed):
        self.peers, self.groups, self.snaps = peers, groups, snaps
        self.halos, self.width, self.cands, self.listed = halos, width, cands, listed
        self.per = snaps // groups
        self.slots = 2 * halos // peers
        self.total = peers * self.slots
        self.data = self.per * self.slots
        self.fit = LANES // listed
        self.codes = -(-(-(-self.data // self.fit)) // groups)
        self.send = self.data + self.codes + (self.data + self.codes) % 2
        self.back = self.data + 1 + (self.data + 1) % 2
        self.half = cands // 2
        self.aligned = self.slots % SUB == 0
        assert snaps % groups == 0 and groups == 2
        assert width == LANES and halos <= LANES and cands <= 512 and cands % WORD == 0
        assert LANES % listed == 0 and self.data <= LANES
        assert peers * groups * self.send % SUB == 0 and peers * groups * self.back % SUB == 0
        assert not self.aligned or (self.codes <= SUB <= self.data)

    def at(self, peer, group, size):
        return (peer * self.groups + group) * size


def order_kernel(plan, out_ref):
    shape = (plan.halos, plan.halos)
    out_ref[...] = jnp.where(iota(shape, 0) < iota(shape, 1), 1.0, 0.0).astype(jnp.bfloat16)


def route_kernel(
    plan, rep_ref, upper_ref, owner_ref, live_ref, cand_ref, span_ref, pick_ref, rows_ref, out_ref, target_ref
):
    n, h, k = plan.peers, plan.halos, plan.listed
    rep = rep_ref[0]
    peer_ids = iota((n, h), 0)
    list_ids = iota((k, h), 0)
    owners = [owner_ref[s : s + 1, :] for s in range(plan.snaps)]
    marks = jnp.concatenate([hot((n, h), 0, o) for o in owners], axis=0)
    prefix = dot(marks, upper_ref[...], 1, 0)
    puts, says, spreads = [], [], []
    for s in range(plan.snaps):
        g, q = s // plan.per, s % plan.per
        mine = jnp.where(peer_ids == owners[s], prefix[s * n : (s + 1) * n], 0.0)
        rank = jnp.sum(mine, axis=0, keepdims=True).astype(jnp.int32)
        live = live_ref[s : s + 1, :] == 1
        place = q * plan.slots + rank
        target_ref[s : s + 1, :] = jnp.where(live, owners[s] * LANES + place, -LANES)
        listing = cand_ref[s]
        pick = pick_ref[s : s + 1, :]
        chosen = jnp.sum(jnp.where(list_ids == pick, listing, 0), axis=0, keepdims=True)
        first = listing[0:1, :]
        kept = jnp.where(list_ids < span_ref[s : s + 1, :], listing, chosen)
        kept = jnp.where(list_ids == pick, first, kept)
        kept = jnp.where(list_ids == 0, chosen, kept)
        code = jnp.where(kept < plan.half, kept - plan.half, kept - plan.half + 1)
        code = code.astype(jnp.float32).astype(jnp.bfloat16)
        spot, line = left(place, plan.fit).astype(jnp.int16), over(place, plan.fit)
        spreads.append(
            jnp.concatenate(
                [jnp.where(jnp.broadcast_to(spot, (k, h)) == b, code, jnp.bfloat16(0)) for b in range(plan.fit)],
                axis=0,
            )
        )
        tells = live & (over(line, plan.codes) == rep)
        line = left(line, plan.codes)
        if plan.aligned:
            puts.append(hot((plan.total, h), 0, jnp.where(live, owners[s] * plan.slots + rank, -1)))
            says.append(hot((n * SUB, h), 0, jnp.where(tells, owners[s] * SUB + line, -1)))
        else:
            base = plan.at(owners[s], g, plan.send)
            shape = (n * plan.groups * plan.send, h)
            puts.append(hot(shape, 0, jnp.where(live, base + place, -1)))
            says.append(hot(shape, 0, jnp.where(tells, base + plan.data + line, -1)))

    def joined(parts, g, axis):
        return jnp.concatenate(parts[g * plan.per : (g + 1) * plan.per], axis=axis)

    tails = [dot(joined(says, g, 1), joined(spreads, g, 1), 1, 1) for g in range(plan.groups)]
    whole = None
    for g in range(plan.groups):
        if plan.aligned:
            tail = tails[g].astype(jnp.bfloat16)
            for q in range(plan.per):
                s = g * plan.per + q
                rows = dot(puts[s], rows_ref[s], 1, 0).astype(jnp.bfloat16)
                for p in range(n):
                    base = plan.at(p, g, plan.send) + q * plan.slots
                    out_ref[base : base + plan.slots, :] = rows[p * plan.slots : (p + 1) * plan.slots]
            for p in range(n):
                base = plan.at(p, g, plan.send)
                out_ref[base + plan.data : base + plan.send, :] = tail[p * SUB : p * SUB + plan.send - plan.data]
        else:
            held_rows = rows_ref[g * plan.per : (g + 1) * plan.per].reshape(plan.per * h, plan.width)
            both = dot(joined(puts, g, 1), held_rows, 1, 0) + tails[g]
            whole = both if whole is None else whole + both
    if not plan.aligned:
        out_ref[...] = whole.astype(jnp.bfloat16)


def soft(v):
    return 1.0 + (jnp.maximum(v, 0.0) + jnp.log1p(jnp.exp(-jnp.abs(v))))


def rows_in(plan, ref, group, q, size):
    if plan.aligned:
        starts = [plan.at(p, group, size) + q * plan.slots for p in range(plan.peers)]
        return jnp.concatenate([ref[a : a + plan.slots, :] for a in starts], axis=0)
    item = iota((plan.total, 1), 0)
    spot = plan.at(over(item, plan.slots), group, size) + q * plan.slots + left(item, plan.slots)
    take = hot((plan.total, plan.peers * plan.groups * size), 1, spot)
    return dot(take, ref[...], 1, 0).astype(jnp.bfloat16)


def tail_in(plan, ref, group, size):
    if plan.aligned:
        ends = [plan.at(p, group, size) + size for p in range(plan.peers)]
        value = jnp.concatenate([ref[a - SUB : a, :] for a in ends], axis=0)
        return value, (lambda p: p * SUB + SUB - (size - plan.data))
    return ref[...], (lambda p: plan.at(p, group, size) + plan.data)


def owner_kernel(plan, rep_ref, got_ref, own_ref, other_ref, peek_ref, out_ref, line_ref, set_ref):
    n, t, c, k = plan.peers, plan.total, plan.cands, plan.listed
    rep = rep_ref[0]
    scale = 1.0 / math.sqrt(plan.width * plan.groups)
    item = iota((1, t), 1)
    source, slot = over(item, plan.slots), left(item, plan.slots)
    snaps, cores = range(plan.per), range(plan.groups)
    ends = [tail_in(plan, got_ref, r, plan.send) for r in cores]

    tables, rows, merits = [], [], []
    for q in snaps:
        own, other = own_ref[rep * plan.per + q], other_ref[rep * plan.per + q]
        pair = [jnp.where(rep == 0, own, other), jnp.where(rep == 0, other, own)]
        tables.append(jnp.concatenate(pair, axis=1))
        rows.append(jnp.concatenate([rows_in(plan, got_ref, r, q, plan.send) for r in cores], axis=1))

    listing = []
    for q in snaps:
        place = q * plan.slots + slot
        spot, line = left(place, plan.fit), over(place, plan.fit)
        wide = None
        for r in cores:
            value, row = ends[r]
            if (q * plan.slots + plan.slots - 1) // plan.fit // plan.codes < r:
                continue
            if q * plan.slots // plan.fit // plan.codes > r:
                continue
            told = jnp.where(over(line, plan.codes) == r, row(source) + left(line, plan.codes), -1)
            piece = dot(value, hot((value.shape[0], t), 0, told), 0, 0)
            wide = piece if wide is None else wide + piece
        codes = wide[0:k]
        for b in range(1, plan.fit):
            codes = jnp.where(spot == b, wide[b * k : (b + 1) * k], codes)
        codes = codes.astype(jnp.int32)
        index = jnp.where(codes < 0, codes + plan.half, codes + plan.half - 1)
        listing.append(jnp.where(codes == 0, -1, index))
        merits.append(dot(tables[q], rows[q], 1, 1))

    words = c // WORD
    word_ids = iota((words, t), 0)
    line_ids = iota((WORD, t), 0)
    bits = jnp.left_shift(jnp.int32(1), line_ids)
    filler = jnp.zeros((SUB - plan.per, t), jnp.float32)
    heads = [listing[q][0:1, :].astype(jnp.float32) for q in snaps]
    heads = jnp.transpose(jnp.concatenate(heads + [filler], axis=0)).astype(jnp.int32)
    descs = [dot(hot((t, c), 1, heads[:, q : q + 1]), tables[q], 1, 0) for q in snaps]
    bests, shares = [], []
    for q in snaps:
        index = listing[q]
        high, bit = index >> 5, jnp.left_shift(jnp.int32(1), index & (WORD - 1))
        line_ref[q, 0], line_ref[q, 1] = high, bit
        sets = jnp.zeros((words, t), jnp.int32)
        for j in range(k):
            sets = sets | jnp.where(line_ref[q, 0, j : j + 1, :] == word_ids, line_ref[q, 1, j : j + 1, :], 0)
        set_ref[q] = sets
        head = index[0:1, :]
        best = jnp.full((WORD, t), NEG, jnp.float32)
        picked = jnp.zeros((WORD, t), jnp.float32)
        rival = jnp.zeros((WORD, t), jnp.float32)
        for w in range(words):
            merit = merits[q][w * WORD : (w + 1) * WORD]
            member = (set_ref[q, w : w + 1, :] & bits) != 0
            listed = jnp.where(member, merit, NEG)
            best = jnp.maximum(best, listed)
            top = jnp.max(listed, axis=1, keepdims=True)
            chosen = line_ids == head - w * WORD
            picked = jnp.where(chosen, merit, picked)
            rival = jnp.where(chosen, top, rival)
        bests.append((jnp.max(best, axis=0, keepdims=True) * scale).astype(jnp.bfloat16))
        mine = soft(jnp.sum(picked, axis=0, keepdims=True) * scale)
        claim = soft(jnp.sum(rival, axis=0, keepdims=True) * scale)
        shares.append(mine / (mine + claim))
    shares = jnp.transpose(jnp.concatenate(shares + [filler], axis=0))

    blends = []
    for q in snaps:
        share = shares[:, q : q + 1]
        blend = (1.0 - share) * rows[q].astype(jnp.float32) + share * descs[q]
        blends.append(blend.astype(jnp.bfloat16))

    tall = SUB if plan.aligned else plan.back
    home = source * tall + (0 if plan.aligned else plan.data)
    here = lax.broadcasted_iota(jnp.int16, (n * tall, t), 0) == home.astype(jnp.int16)
    lines = [jnp.where(here, bests[q], jnp.bfloat16(0)) for q in snaps]
    slot_of = left(iota((t, 1), 0), plan.slots)
    lanes = [hot((t, LANES), 1, q * plan.slots + slot_of) for q in snaps]
    tail = dot(jnp.concatenate(lines, axis=1), jnp.concatenate(lanes, axis=0), 1, 0).astype(jnp.bfloat16)
    width = plan.width
    if plan.aligned:
        for r in cores:
            for p in range(n):
                base = plan.at(p, r, plan.back)
                for q in snaps:
                    a = base + q * plan.slots
                    out_ref[a : a + plan.slots, :] = blends[q][
                        p * plan.slots : (p + 1) * plan.slots, r * width : (r + 1) * width
                    ]
                out_ref[base + plan.data : base + plan.back, :] = tail[p * SUB : p * SUB + plan.back - plan.data]
        return
    height = n * plan.groups * plan.back
    col = iota((1, n * tall), 1)
    full = None
    for r in cores:
        piece = dot(hot((height, n * tall), 0, plan.at(col // tall, r, tall) + col % tall), tail, 1, 0)
        for q in snaps:
            put = hot((height, t), 0, plan.at(source, r, plan.back) + q * plan.slots + slot)
            piece = piece + dot(put, blends[q][:, r * width : (r + 1) * width], 1, 0)
        full = piece if full is None else full + piece
    out_ref[...] = full.astype(jnp.bfloat16)


def land_kernel(plan, back_ref, target_ref, rows_ref, out_ref, best_ref):
    h, t = plan.halos, plan.total
    target = target_ref[...]
    column = jnp.transpose(target)
    for g in range(plan.groups):
        tail, row = tail_in(plan, back_ref, g, plan.back)
        pulls = []
        for q in range(plan.per):
            s = g * plan.per + q
            spot = column[:, s : s + 1]
            owner, slot = spot >> 7, (spot & (LANES - 1)) - q * plan.slots
            take = hot((h, t), 1, jnp.where(spot >= 0, owner * plan.slots + slot, -1))
            rows = dot(take, rows_in(plan, back_ref, g, q, plan.back), 1, 0)
            rows = jnp.where(jnp.broadcast_to(spot, (h, plan.width)) >= 0, rows, rows_ref[s].astype(jnp.float32))
            out_ref[s] = rows.astype(jnp.bfloat16)
            spot = target[s : s + 1, :]
            pulls.append(hot((tail.shape[0], h), 0, jnp.where(spot >= 0, row(spot >> 7), -1)))
        grid = dot(tail, jnp.concatenate(pulls, axis=1), 0, 0)
        for q in range(plan.per):
            s = g * plan.per + q
            place = target[s : s + 1, :] & (LANES - 1)
            mine = jnp.where(iota((LANES, h), 0) == place, grid[:, q * h : (q + 1) * h], 0.0)
            best_ref[s : s + 1, :] = jnp.sum(mine, axis=0, keepdims=True).astype(jnp.bfloat16)


def body(halo_rows, unmatched, owner_id, cand_index, lengths, choice_index, desc_rows):
    peers, groups = lax.axis_size("space"), lax.axis_size("rep")
    snaps, halos, width = halo_rows.shape
    cands, listed = desc_rows.shape[1], cand_index.shape[2]
    plan = Plan(peers, groups, snaps, halos, width, cands, listed)
    rep = lax.axis_index("rep").astype(jnp.int32)

    def swap(flat, size):
        boxed = flat.reshape(peers * groups, size // 2, 2, width)
        boxed = lax.all_to_all(boxed, ("space", "rep"), 0, 0, tiled=True)
        return boxed.reshape(peers * groups * size, width)

    other = lax.ppermute(desc_rows, "rep", [(0, 1), (1, 0)])

    vmem = pl.BlockSpec(memory_space=pltpu.VMEM)
    smem = pl.BlockSpec(memory_space=pltpu.SMEM)
    hbm = pl.BlockSpec(memory_space=pltpu.HBM)
    small = pltpu.CompilerParams(vmem_limit_bytes=20 << 20)
    packed = pltpu.CompilerParams(vmem_limit_bytes=20 << 20)
    flat = (snaps, halos)
    upper = pl.pallas_call(
        lambda *refs: order_kernel(plan, *refs),
        name="order",
        compiler_params=pltpu.CompilerParams(vmem_limit_bytes=66_600_000),
        cost_estimate=pl.CostEstimate(flops=1 << 32, bytes_accessed=0, transcendentals=0),
        out_shape=pltpu.VMEM((halos, halos), jnp.bfloat16),
        out_specs=vmem,
    )()
    sent, target = pl.pallas_call(
        lambda *refs: route_kernel(plan, *refs),
        name="route",
        compiler_params=small,
        out_shape=(
            jax.ShapeDtypeStruct((peers * groups * plan.send, width), jnp.bfloat16),
            jax.ShapeDtypeStruct(flat, jnp.int32),
        ),
        in_specs=[smem] + [vmem] * 7,
        out_specs=(vmem, vmem),
    )(
        rep.reshape(1),
        upper,
        owner_id.reshape(flat),
        unmatched,
        jnp.swapaxes(cand_index, 1, 2),
        lengths,
        choice_index,
        halo_rows,
    )
    got = swap(sent, plan.send)
    peek = got[0:SUB] * jnp.bfloat16(2)
    reply = pl.pallas_call(
        lambda *refs: owner_kernel(plan, *refs),
        name="owner",
        compiler_params=packed,
        out_shape=jax.ShapeDtypeStruct((peers * groups * plan.back, width), jnp.bfloat16),
        in_specs=[smem, vmem, vmem, vmem, vmem],
        out_specs=vmem,
        scratch_shapes=[
            pltpu.VMEM((plan.per, 2, listed, plan.total), jnp.int32),
            pltpu.VMEM((plan.per, cands // WORD, plan.total), jnp.int32),
        ],
    )(rep.reshape(1), got, desc_rows, other, peek)
    back = swap(reply, plan.back)
    return pl.pallas_call(
        lambda *refs: land_kernel(plan, *refs),
        name="land",
        compiler_params=packed,
        out_shape=(
            jax.ShapeDtypeStruct((snaps, halos, width), jnp.bfloat16),
            jax.ShapeDtypeStruct((snaps, halos), jnp.bfloat16),
        ),
        in_specs=[vmem] * 3,
        out_specs=(vmem, vmem),
    )(back, target, halo_rows)


def solution(mesh):
    in_specs = (
        P(None, "space", "rep"),
        P(None, "space"),
        P(None, "space", None),
        P(None, "space", None),
        P(None, "space"),
        P(None, "space"),
        P(None, "space", "rep"),
    )
    out_specs = (P(None, "space", "rep"), P(None, "space"))

    return jax.shard_map(body, mesh=mesh, in_specs=in_specs, out_specs=out_specs, check_vma=False)
```

```python
import math

import jax
import jax.numpy as jnp
from jax import lax
from jax.experimental import pallas as pl
from jax.experimental.pallas import tpu as pltpu
from jax.sharding import PartitionSpec as P

LANES = 128
SUB = 8
WORD = 32
NEG = -3.0e38


def iota(shape, axis):
    return lax.broadcasted_iota(jnp.int32, shape, axis)


def over(x, m):
    return x >> (m.bit_length() - 1) if m & (m - 1) == 0 else x // m


def left(x, m):
    return x & (m - 1) if m & (m - 1) == 0 else x % m


def hot(shape, axis, spot):
    mask = lax.broadcasted_iota(jnp.int16, shape, axis) == spot.astype(jnp.int16)
    return jnp.where(mask, jnp.bfloat16(1), jnp.bfloat16(0))


def dot(a, b, ca, cb):
    return lax.dot_general(a, b, (((ca,), (cb,)), ((), ())), preferred_element_type=jnp.float32)


class Plan:
    def __init__(self, peers, groups, snaps, halos, width, cands, listed):
        self.peers, self.groups, self.snaps = peers, groups, snaps
        self.halos, self.width, self.cands, self.listed = halos, width, cands, listed
        self.per = snaps // groups
        self.slots = 2 * halos // peers
        self.total = peers * self.slots
        self.data = self.per * self.slots
        self.fit = LANES // listed
        self.codes = -(-(-(-self.data // self.fit)) // groups)
        self.send = self.data + self.codes + (self.data + self.codes) % 2
        self.back = self.data + 1 + (self.data + 1) % 2
        self.half = cands // 2
        self.aligned = self.slots % SUB == 0
        assert snaps % groups == 0 and groups == 2
        assert width == LANES and halos <= LANES and cands <= 512 and cands % WORD == 0
        assert LANES % listed == 0 and self.data <= LANES
        assert peers * groups * self.send % SUB == 0 and peers * groups * self.back % SUB == 0
        assert not self.aligned or (self.codes <= SUB <= self.data)

    def at(self, peer, group, size):
        return (peer * self.groups + group) * size


def order_kernel(plan, out_ref):
    shape = (plan.halos, plan.halos)
    out_ref[...] = jnp.where(iota(shape, 0) < iota(shape, 1), 1.0, 0.0).astype(jnp.bfloat16)


def route_kernel(
    plan, rep_ref, upper_ref, owner_ref, live_ref, cand_ref, span_ref, pick_ref, rows_ref, out_ref, target_ref
):
    n, h, k = plan.peers, plan.halos, plan.listed
    rep = rep_ref[0]
    peer_ids = iota((n, h), 0)
    list_ids = iota((k, h), 0)
    owners = [owner_ref[s : s + 1, :] for s in range(plan.snaps)]
    marks = jnp.concatenate([hot((n, h), 0, o) for o in owners], axis=0)
    prefix = dot(marks, upper_ref[...], 1, 0)
    puts, says, spreads = [], [], []
    for s in range(plan.snaps):
        g, q = s // plan.per, s % plan.per
        mine = jnp.where(peer_ids == owners[s], prefix[s * n : (s + 1) * n], 0.0)
        rank = jnp.sum(mine, axis=0, keepdims=True).astype(jnp.int32)
        live = live_ref[s : s + 1, :] == 1
        place = q * plan.slots + rank
        target_ref[s : s + 1, :] = jnp.where(live, owners[s] * LANES + place, -LANES)
        listing = cand_ref[s]
        pick = pick_ref[s : s + 1, :]
        chosen = jnp.sum(jnp.where(list_ids == pick, listing, 0), axis=0, keepdims=True)
        first = listing[0:1, :]
        kept = jnp.where(list_ids < span_ref[s : s + 1, :], listing, chosen)
        kept = jnp.where(list_ids == pick, first, kept)
        kept = jnp.where(list_ids == 0, chosen, kept)
        code = jnp.where(kept < plan.half, kept - plan.half, kept - plan.half + 1)
        code = code.astype(jnp.float32).astype(jnp.bfloat16)
        spot, line = left(place, plan.fit).astype(jnp.int16), over(place, plan.fit)
        spreads.append(
            jnp.concatenate(
                [jnp.where(jnp.broadcast_to(spot, (k, h)) == b, code, jnp.bfloat16(0)) for b in range(plan.fit)],
                axis=0,
            )
        )
        tells = live & (over(line, plan.codes) == rep)
        line = left(line, plan.codes)
        if plan.aligned:
            puts.append(hot((plan.total, h), 0, jnp.where(live, owners[s] * plan.slots + rank, -1)))
            says.append(hot((n * SUB, h), 0, jnp.where(tells, owners[s] * SUB + line, -1)))
        else:
            base = plan.at(owners[s], g, plan.send)
            shape = (n * plan.groups * plan.send, h)
            puts.append(hot(shape, 0, jnp.where(live, base + place, -1)))
            says.append(hot(shape, 0, jnp.where(tells, base + plan.data + line, -1)))

    def joined(parts, g, axis):
        return jnp.concatenate(parts[g * plan.per : (g + 1) * plan.per], axis=axis)

    tails = [dot(joined(says, g, 1), joined(spreads, g, 1), 1, 1) for g in range(plan.groups)]
    whole = None
    for g in range(plan.groups):
        if plan.aligned:
            tail = tails[g].astype(jnp.bfloat16)
            for q in range(plan.per):
                s = g * plan.per + q
                rows = dot(puts[s], rows_ref[s], 1, 0).astype(jnp.bfloat16)
                for p in range(n):
                    base = plan.at(p, g, plan.send) + q * plan.slots
                    out_ref[base : base + plan.slots, :] = rows[p * plan.slots : (p + 1) * plan.slots]
            for p in range(n):
                base = plan.at(p, g, plan.send)
                out_ref[base + plan.data : base + plan.send, :] = tail[p * SUB : p * SUB + plan.send - plan.data]
        else:
            held_rows = rows_ref[g * plan.per : (g + 1) * plan.per].reshape(plan.per * h, plan.width)
            both = dot(joined(puts, g, 1), held_rows, 1, 0) + tails[g]
            whole = both if whole is None else whole + both
    if not plan.aligned:
        out_ref[...] = whole.astype(jnp.bfloat16)


def soft(v):
    return 1.0 + (jnp.maximum(v, 0.0) + jnp.log1p(jnp.exp(-jnp.abs(v))))


def rows_in(plan, ref, group, q, size):
    if plan.aligned:
        starts = [plan.at(p, group, size) + q * plan.slots for p in range(plan.peers)]
        return jnp.concatenate([ref[a : a + plan.slots, :] for a in starts], axis=0)
    item = iota((plan.total, 1), 0)
    spot = plan.at(over(item, plan.slots), group, size) + q * plan.slots + left(item, plan.slots)
    take = hot((plan.total, plan.peers * plan.groups * size), 1, spot)
    return dot(take, ref[...], 1, 0).astype(jnp.bfloat16)


def tail_in(plan, ref, group, size):
    if plan.aligned:
        ends = [plan.at(p, group, size) + size for p in range(plan.peers)]
        value = jnp.concatenate([ref[a - SUB : a, :] for a in ends], axis=0)
        return value, (lambda p: p * SUB + SUB - (size - plan.data))
    return ref[...], (lambda p: plan.at(p, group, size) + plan.data)


def owner_kernel(plan, rep_ref, got_ref, own_ref, other_ref, peek_ref, out_ref, line_ref, set_ref):
    n, t, c, k = plan.peers, plan.total, plan.cands, plan.listed
    rep = rep_ref[0]
    scale = 1.0 / math.sqrt(plan.width * plan.groups)
    item = iota((1, t), 1)
    source, slot = over(item, plan.slots), left(item, plan.slots)
    snaps, cores = range(plan.per), range(plan.groups)
    ends = [tail_in(plan, got_ref, r, plan.send) for r in cores]

    tables, rows, merits = [], [], []
    for q in snaps:
        own, other = own_ref[rep * plan.per + q], other_ref[rep * plan.per + q]
        pair = [jnp.where(rep == 0, own, other), jnp.where(rep == 0, other, own)]
        tables.append(jnp.concatenate(pair, axis=1))
        rows.append(jnp.concatenate([rows_in(plan, got_ref, r, q, plan.send) for r in cores], axis=1))

    listing = []
    for q in snaps:
        place = q * plan.slots + slot
        spot, line = left(place, plan.fit), over(place, plan.fit)
        wide = None
        for r in cores:
            value, row = ends[r]
            if (q * plan.slots + plan.slots - 1) // plan.fit // plan.codes < r:
                continue
            if q * plan.slots // plan.fit // plan.codes > r:
                continue
            told = jnp.where(over(line, plan.codes) == r, row(source) + left(line, plan.codes), -1)
            piece = dot(value, hot((value.shape[0], t), 0, told), 0, 0)
            wide = piece if wide is None else wide + piece
        codes = wide[0:k]
        for b in range(1, plan.fit):
            codes = jnp.where(spot == b, wide[b * k : (b + 1) * k], codes)
        codes = codes.astype(jnp.int32)
        index = jnp.where(codes < 0, codes + plan.half, codes + plan.half - 1)
        listing.append(jnp.where(codes == 0, -1, index))
        merits.append(dot(tables[q], rows[q], 1, 1))

    words = c // WORD
    word_ids = iota((words, t), 0)
    line_ids = iota((WORD, t), 0)
    bits = jnp.left_shift(jnp.int32(1), line_ids)
    filler = jnp.zeros((SUB - plan.per, t), jnp.float32)
    heads = [listing[q][0:1, :].astype(jnp.float32) for q in snaps]
    heads = jnp.transpose(jnp.concatenate(heads + [filler], axis=0)).astype(jnp.int32)
    descs = [dot(hot((t, c), 1, heads[:, q : q + 1]), tables[q], 1, 0) for q in snaps]
    bests, shares = [], []
    for q in snaps:
        index = listing[q]
        high, bit = index >> 5, jnp.left_shift(jnp.int32(1), index & (WORD - 1))
        line_ref[q, 0], line_ref[q, 1] = high, bit
        sets = jnp.zeros((words, t), jnp.int32)
        for j in range(k):
            sets = sets | jnp.where(line_ref[q, 0, j : j + 1, :] == word_ids, line_ref[q, 1, j : j + 1, :], 0)
        set_ref[q] = sets
        head = index[0:1, :]
        strip_of = jnp.where(line_ids[0:SUB] == (head & (SUB - 1)), head >> 3, -1)
        best = jnp.full((SUB, t), NEG, jnp.float32)
        picked = jnp.zeros((SUB, t), jnp.float32)
        rival = jnp.zeros((SUB, t), jnp.float32)
        for w in range(words):
            for i in range(WORD // SUB):
                a = i * SUB
                merit = merits[q][w * WORD + a : w * WORD + a + SUB]
                member = (set_ref[q, w : w + 1, :] & bits[a : a + SUB]) != 0
                listed = jnp.where(member, merit, NEG)
                best = jnp.maximum(best, listed)
                top = jnp.max(listed, axis=1, keepdims=True)
                chosen = strip_of == (w * WORD + a) // SUB
                picked = jnp.where(chosen, merit, picked)
                rival = jnp.where(chosen, top, rival)
        bests.append((jnp.max(best, axis=0, keepdims=True) * scale).astype(jnp.bfloat16))
        mine = soft(jnp.sum(picked, axis=0, keepdims=True) * scale)
        claim = soft(jnp.sum(rival, axis=0, keepdims=True) * scale)
        shares.append(mine / (mine + claim))
    shares = jnp.transpose(jnp.concatenate(shares + [filler], axis=0))

    blends = []
    for q in snaps:
        share = shares[:, q : q + 1]
        mine = rows[q].astype(jnp.float32)
        blend = mine + share * (descs[q] - mine)
        blends.append(blend.astype(jnp.bfloat16))

    tall = SUB if plan.aligned else plan.back
    home = source * tall + (0 if plan.aligned else plan.data)
    here = lax.broadcasted_iota(jnp.int16, (n * tall, t), 0) == home.astype(jnp.int16)
    lines = [jnp.where(here, bests[q], jnp.bfloat16(0)) for q in snaps]
    slot_of = left(iota((t, 1), 0), plan.slots)
    lanes = [hot((t, LANES), 1, q * plan.slots + slot_of) for q in snaps]
    tail = dot(jnp.concatenate(lines, axis=1), jnp.concatenate(lanes, axis=0), 1, 0).astype(jnp.bfloat16)
    width = plan.width
    if plan.aligned:
        for r in cores:
            for p in range(n):
                base = plan.at(p, r, plan.back)
                for q in snaps:
                    a = base + q * plan.slots
                    out_ref[a : a + plan.slots, :] = blends[q][
                        p * plan.slots : (p + 1) * plan.slots, r * width : (r + 1) * width
                    ]
                out_ref[base + plan.data : base + plan.back, :] = tail[p * SUB : p * SUB + plan.back - plan.data]
        return
    height = n * plan.groups * plan.back
    col = iota((1, n * tall), 1)
    full = None
    for r in cores:
        piece = dot(hot((height, n * tall), 0, plan.at(col // tall, r, tall) + col % tall), tail, 1, 0)
        for q in snaps:
            put = hot((height, t), 0, plan.at(source, r, plan.back) + q * plan.slots + slot)
            piece = piece + dot(put, blends[q][:, r * width : (r + 1) * width], 1, 0)
        full = piece if full is None else full + piece
    out_ref[...] = full.astype(jnp.bfloat16)


def land_kernel(plan, back_ref, target_ref, rows_ref, out_ref, best_ref):
    h, t = plan.halos, plan.total
    target = target_ref[...]
    column = jnp.transpose(target)
    for g in range(plan.groups):
        tail, row = tail_in(plan, back_ref, g, plan.back)
        pulls = []
        for q in range(plan.per):
            s = g * plan.per + q
            spot = column[:, s : s + 1]
            owner, slot = spot >> 7, (spot & (LANES - 1)) - q * plan.slots
            take = hot((h, t), 1, jnp.where(spot >= 0, owner * plan.slots + slot, -1))
            rows = dot(take, rows_in(plan, back_ref, g, q, plan.back), 1, 0)
            rows = jnp.where(jnp.broadcast_to(spot, (h, plan.width)) >= 0, rows, rows_ref[s].astype(jnp.float32))
            out_ref[s] = rows.astype(jnp.bfloat16)
            spot = target[s : s + 1, :]
            pulls.append(hot((tail.shape[0], h), 0, jnp.where(spot >= 0, row(spot >> 7), -1)))
        grid = dot(tail, jnp.concatenate(pulls, axis=1), 0, 0)
        for q in range(plan.per):
            s = g * plan.per + q
            place = target[s : s + 1, :] & (LANES - 1)
            mine = jnp.where(iota((LANES, h), 0) == place, grid[:, q * h : (q + 1) * h], 0.0)
            best_ref[s : s + 1, :] = jnp.sum(mine, axis=0, keepdims=True).astype(jnp.bfloat16)


def body(halo_rows, unmatched, owner_id, cand_index, lengths, choice_index, desc_rows):
    peers, groups = lax.axis_size("space"), lax.axis_size("rep")
    snaps, halos, width = halo_rows.shape
    cands, listed = desc_rows.shape[1], cand_index.shape[2]
    plan = Plan(peers, groups, snaps, halos, width, cands, listed)
    rep = lax.axis_index("rep").astype(jnp.int32)

    def swap(flat, size):
        boxed = flat.reshape(peers * groups, size // 2, 2, width)
        boxed = lax.all_to_all(boxed, ("space", "rep"), 0, 0, tiled=True)
        return boxed.reshape(peers * groups * size, width)

    other = lax.ppermute(desc_rows, "rep", [(0, 1), (1, 0)])

    vmem = pl.BlockSpec(memory_space=pltpu.VMEM)
    smem = pl.BlockSpec(memory_space=pltpu.SMEM)
    hbm = pl.BlockSpec(memory_space=pltpu.HBM)
    small = pltpu.CompilerParams(vmem_limit_bytes=20 << 20)
    packed = pltpu.CompilerParams(vmem_limit_bytes=20 << 20)
    flat = (snaps, halos)
    upper = pl.pallas_call(
        lambda *refs: order_kernel(plan, *refs),
        name="order",
        compiler_params=pltpu.CompilerParams(vmem_limit_bytes=66_600_000),
        cost_estimate=pl.CostEstimate(flops=1 << 32, bytes_accessed=0, transcendentals=0),
        out_shape=pltpu.VMEM((halos, halos), jnp.bfloat16),
        out_specs=vmem,
    )()
    sent, target = pl.pallas_call(
        lambda *refs: route_kernel(plan, *refs),
        name="route",
        compiler_params=small,
        out_shape=(
            jax.ShapeDtypeStruct((peers * groups * plan.send, width), jnp.bfloat16),
            jax.ShapeDtypeStruct(flat, jnp.int32),
        ),
        in_specs=[smem] + [vmem] * 7,
        out_specs=(vmem, vmem),
    )(
        rep.reshape(1),
        upper,
        owner_id.reshape(flat),
        unmatched,
        jnp.swapaxes(cand_index, 1, 2),
        lengths,
        choice_index,
        halo_rows,
    )
    got = swap(sent, plan.send)
    peek = got[0:SUB] * jnp.bfloat16(2)
    reply = pl.pallas_call(
        lambda *refs: owner_kernel(plan, *refs),
        name="owner",
        compiler_params=packed,
        out_shape=jax.ShapeDtypeStruct((peers * groups * plan.back, width), jnp.bfloat16),
        in_specs=[smem, vmem, vmem, vmem, vmem],
        out_specs=vmem,
        scratch_shapes=[
            pltpu.VMEM((plan.per, 2, listed, plan.total), jnp.int32),
            pltpu.VMEM((plan.per, cands // WORD, plan.total), jnp.int32),
        ],
    )(rep.reshape(1), got, desc_rows, other, peek)
    back = swap(reply, plan.back)
    return pl.pallas_call(
        lambda *refs: land_kernel(plan, *refs),
        name="land",
        compiler_params=packed,
        out_shape=(
            jax.ShapeDtypeStruct((snaps, halos, width), jnp.bfloat16),
            jax.ShapeDtypeStruct((snaps, halos), jnp.bfloat16),
        ),
        in_specs=[vmem] * 3,
        out_specs=(vmem, vmem),
    )(back, target, halo_rows)


def solution(mesh):
    in_specs = (
        P(None, "space", "rep"),
        P(None, "space"),
        P(None, "space", None),
        P(None, "space", None),
        P(None, "space"),
        P(None, "space"),
        P(None, "space", "rep"),
    )
    out_specs = (P(None, "space", "rep"), P(None, "space"))

    return jax.shard_map(body, mesh=mesh, in_specs=in_specs, out_specs=out_specs, check_vma=False)
```

```python
import math

import jax
import jax.numpy as jnp
from jax import lax
from jax.experimental import pallas as pl
from jax.experimental.pallas import tpu as pltpu
from jax.sharding import PartitionSpec as P

LANES = 128
SUB = 8
WORD = 32
NEG = -3.0e38


def iota(shape, axis):
    return lax.broadcasted_iota(jnp.int32, shape, axis)


def over(x, m):
    return x >> (m.bit_length() - 1) if m & (m - 1) == 0 else x // m


def left(x, m):
    return x & (m - 1) if m & (m - 1) == 0 else x % m


def hot(shape, axis, spot):
    mask = lax.broadcasted_iota(jnp.int16, shape, axis) == spot.astype(jnp.int16)
    return jnp.where(mask, jnp.bfloat16(1), jnp.bfloat16(0))


def dot(a, b, ca, cb):
    return lax.dot_general(a, b, (((ca,), (cb,)), ((), ())), preferred_element_type=jnp.float32)


class Plan:
    def __init__(self, peers, groups, snaps, halos, width, cands, listed):
        self.peers, self.groups, self.snaps = peers, groups, snaps
        self.halos, self.width, self.cands, self.listed = halos, width, cands, listed
        self.per = snaps // groups
        self.slots = 2 * halos // peers
        self.total = peers * self.slots
        self.data = self.per * self.slots
        self.fit = LANES // listed
        self.codes = -(-(-(-self.data // self.fit)) // groups)
        self.send = self.data + self.codes + (self.data + self.codes) % 2
        self.back = self.data + 1 + (self.data + 1) % 2
        self.half = cands // 2
        self.aligned = self.slots % SUB == 0
        assert snaps % groups == 0 and groups == 2
        assert width == LANES and halos <= LANES and cands <= 512 and cands % WORD == 0
        assert LANES % listed == 0 and self.data <= LANES
        assert peers * groups * self.send % SUB == 0 and peers * groups * self.back % SUB == 0
        assert not self.aligned or (self.codes <= SUB <= self.data)

    def at(self, peer, group, size):
        return (peer * self.groups + group) * size


def order_kernel(plan, out_ref):
    shape = (plan.halos, plan.halos)
    out_ref[...] = jnp.where(iota(shape, 0) < iota(shape, 1), 1.0, 0.0).astype(jnp.bfloat16)


def route_kernel(
    plan, rep_ref, upper_ref, owner_ref, live_ref, cand_ref, span_ref, pick_ref, rows_ref, out_ref, target_ref
):
    n, h, k = plan.peers, plan.halos, plan.listed
    rep = rep_ref[0]
    peer_ids = iota((n, h), 0)
    list_ids = iota((k, h), 0)
    owners = [owner_ref[s : s + 1, :] for s in range(plan.snaps)]
    marks = jnp.concatenate([hot((n, h), 0, o) for o in owners], axis=0)
    prefix = dot(marks, upper_ref[...], 1, 0)
    puts, says, spreads, pieces = [], [], [], []
    for s in range(plan.snaps):
        g, q = s // plan.per, s % plan.per
        mine = jnp.where(peer_ids == owners[s], prefix[s * n : (s + 1) * n], 0.0)
        rank = jnp.sum(mine, axis=0, keepdims=True).astype(jnp.int32)
        live = live_ref[s : s + 1, :] == 1
        place = q * plan.slots + rank
        target_ref[s : s + 1, :] = jnp.where(live, owners[s] * LANES + place, -LANES)
        listing = cand_ref[s]
        pick = pick_ref[s : s + 1, :]
        chosen = jnp.sum(jnp.where(list_ids == pick, listing, 0), axis=0, keepdims=True)
        first = listing[0:1, :]
        kept = jnp.where(list_ids < span_ref[s : s + 1, :], listing, chosen)
        kept = jnp.where(list_ids == pick, first, kept)
        kept = jnp.where(list_ids == 0, chosen, kept)
        code = jnp.where(kept < plan.half, kept - plan.half, kept - plan.half + 1)
        pieces.append((place, code.astype(jnp.float32), jnp.where(live, owners[s], -1)))
        if plan.aligned:
            puts.append(hot((plan.total, h), 0, jnp.where(live, owners[s] * plan.slots + rank, -1)))
        else:
            base = plan.at(owners[s], g, plan.send)
            shape = (n * plan.groups * plan.send, h)
            puts.append(hot(shape, 0, jnp.where(live, base + place, -1)))

    single = plan.per == plan.groups == 2 and plan.slots == plan.codes * plan.fit
    for g in range(plan.groups):
        mine = pieces[g * plan.per : (g + 1) * plan.per]
        if single:
            mine = [tuple(jnp.where(rep == 0, x, y) for x, y in zip(*mine))]
        for place, code, owner in mine:
            spot, line = left(place, plan.fit).astype(jnp.int16), over(place, plan.fit)
            spot, code = jnp.broadcast_to(spot, (k, h)), code.astype(jnp.bfloat16)
            spreads.append(
                jnp.concatenate([jnp.where(spot == b, code, jnp.bfloat16(0)) for b in range(plan.fit)], axis=0)
            )
            tells = (owner >= 0) & (over(line, plan.codes) == rep)
            line = left(line, plan.codes)
            if plan.aligned:
                says.append(hot((n * SUB, h), 0, jnp.where(tells, owner * SUB + line, -1)))
            else:
                row = plan.at(owner, g, plan.send) + plan.data + line
                says.append(hot((n * plan.groups * plan.send, h), 0, jnp.where(tells, row, -1)))

    def joined(parts, g, axis):
        return jnp.concatenate(parts[g * plan.per : (g + 1) * plan.per], axis=axis)

    each = len(says) // plan.groups
    tails = []
    for g in range(plan.groups):
        pair = [jnp.concatenate(x[g * each : (g + 1) * each], axis=1) for x in (says, spreads)]
        tails.append(dot(*pair, 1, 1))
    whole = None
    for g in range(plan.groups):
        if plan.aligned:
            tail = tails[g].astype(jnp.bfloat16)
            for q in range(plan.per):
                s = g * plan.per + q
                rows = dot(puts[s], rows_ref[s], 1, 0).astype(jnp.bfloat16)
                for p in range(n):
                    base = plan.at(p, g, plan.send) + q * plan.slots
                    out_ref[base : base + plan.slots, :] = rows[p * plan.slots : (p + 1) * plan.slots]
            for p in range(n):
                base = plan.at(p, g, plan.send)
                out_ref[base + plan.data : base + plan.send, :] = tail[p * SUB : p * SUB + plan.send - plan.data]
        else:
            held_rows = rows_ref[g * plan.per : (g + 1) * plan.per].reshape(plan.per * h, plan.width)
            both = dot(joined(puts, g, 1), held_rows, 1, 0) + tails[g]
            whole = both if whole is None else whole + both
    if not plan.aligned:
        out_ref[...] = whole.astype(jnp.bfloat16)


def soft(v):
    return 1.0 + (jnp.maximum(v, 0.0) + jnp.log1p(jnp.exp(-jnp.abs(v))))


def rows_in(plan, ref, group, q, size):
    if plan.aligned:
        starts = [plan.at(p, group, size) + q * plan.slots for p in range(plan.peers)]
        return jnp.concatenate([ref[a : a + plan.slots, :] for a in starts], axis=0)
    item = iota((plan.total, 1), 0)
    spot = plan.at(over(item, plan.slots), group, size) + q * plan.slots + left(item, plan.slots)
    take = hot((plan.total, plan.peers * plan.groups * size), 1, spot)
    return dot(take, ref[...], 1, 0).astype(jnp.bfloat16)


def tail_in(plan, ref, group, size):
    if plan.aligned:
        ends = [plan.at(p, group, size) + size for p in range(plan.peers)]
        value = jnp.concatenate([ref[a - SUB : a, :] for a in ends], axis=0)
        return value, (lambda p: p * SUB + SUB - (size - plan.data))
    return ref[...], (lambda p: plan.at(p, group, size) + plan.data)


def owner_kernel(plan, rep_ref, got_ref, own_ref, other_ref, peek_ref, out_ref, line_ref, set_ref):
    n, t, c, k = plan.peers, plan.total, plan.cands, plan.listed
    rep = rep_ref[0]
    scale = 1.0 / math.sqrt(plan.width * plan.groups)
    item = iota((1, t), 1)
    source, slot = over(item, plan.slots), left(item, plan.slots)
    snaps, cores = range(plan.per), range(plan.groups)
    ends = [tail_in(plan, got_ref, r, plan.send) for r in cores]

    tables, rows, merits = [], [], []
    for q in snaps:
        own, other = own_ref[rep * plan.per + q], other_ref[rep * plan.per + q]
        pair = [jnp.where(rep == 0, own, other), jnp.where(rep == 0, other, own)]
        tables.append(jnp.concatenate(pair, axis=1))
        rows.append(jnp.concatenate([rows_in(plan, got_ref, r, q, plan.send) for r in cores], axis=1))

    listing = []
    for q in snaps:
        place = q * plan.slots + slot
        spot, line = left(place, plan.fit), over(place, plan.fit)
        wide = None
        for r in cores:
            value, row = ends[r]
            if (q * plan.slots + plan.slots - 1) // plan.fit // plan.codes < r:
                continue
            if q * plan.slots // plan.fit // plan.codes > r:
                continue
            told = jnp.where(over(line, plan.codes) == r, row(source) + left(line, plan.codes), -1)
            piece = dot(value, hot((value.shape[0], t), 0, told), 0, 0)
            wide = piece if wide is None else wide + piece
        codes = wide[0:k]
        for b in range(1, plan.fit):
            codes = jnp.where(spot == b, wide[b * k : (b + 1) * k], codes)
        codes = codes.astype(jnp.int32)
        index = jnp.where(codes < 0, codes + plan.half, codes + plan.half - 1)
        listing.append(jnp.where(codes == 0, -1, index))
        merits.append(dot(tables[q], rows[q], 1, 1))

    words = c // WORD
    word_ids = iota((words, t), 0)
    line_ids = iota((WORD, t), 0)
    bits = jnp.left_shift(jnp.int32(1), line_ids)
    filler = jnp.zeros((SUB - plan.per, t), jnp.float32)
    heads = [listing[q][0:1, :].astype(jnp.float32) for q in snaps]
    heads = jnp.transpose(jnp.concatenate(heads + [filler], axis=0)).astype(jnp.int32)
    descs = [dot(hot((t, c), 1, heads[:, q : q + 1]), tables[q], 1, 0) for q in snaps]
    bests, shares = [], []
    for q in snaps:
        index = listing[q]
        high, bit = index >> 5, jnp.left_shift(jnp.int32(1), index & (WORD - 1))
        line_ref[q, 0], line_ref[q, 1] = high, bit
        sets = jnp.zeros((words, t), jnp.int32)
        for j in range(k):
            sets = sets | jnp.where(line_ref[q, 0, j : j + 1, :] == word_ids, line_ref[q, 1, j : j + 1, :], 0)
        set_ref[q] = sets
        head = index[0:1, :]
        strip_of = jnp.where(line_ids[0:SUB] == (head & (SUB - 1)), head >> 3, -1)
        best = jnp.full((SUB, t), NEG, jnp.float32)
        picked = jnp.zeros((SUB, t), jnp.float32)
        rival = jnp.zeros((SUB, t), jnp.float32)
        for w in range(words):
            for i in range(WORD // SUB):
                a = i * SUB
                merit = merits[q][w * WORD + a : w * WORD + a + SUB]
                member = (set_ref[q, w : w + 1, :] & bits[a : a + SUB]) != 0
                listed = jnp.where(member, merit, NEG)
                best = jnp.maximum(best, listed)
                top = jnp.max(listed, axis=1, keepdims=True)
                chosen = strip_of == (w * WORD + a) // SUB
                picked = jnp.where(chosen, merit, picked)
                rival = jnp.where(chosen, top, rival)
        bests.append((jnp.max(best, axis=0, keepdims=True) * scale).astype(jnp.bfloat16))
        mine = soft(jnp.sum(picked, axis=0, keepdims=True) * scale)
        claim = soft(jnp.sum(rival, axis=0, keepdims=True) * scale)
        shares.append(mine / (mine + claim))
    shares = jnp.transpose(jnp.concatenate(shares + [filler], axis=0))

    blends = []
    for q in snaps:
        share = shares[:, q : q + 1]
        mine = rows[q].astype(jnp.float32)
        blend = mine + share * (descs[q] - mine)
        blends.append(blend.astype(jnp.bfloat16))

    tall = SUB if plan.aligned else plan.back
    home = source * tall + (0 if plan.aligned else plan.data)
    here = lax.broadcasted_iota(jnp.int16, (n * tall, t), 0) == home.astype(jnp.int16)
    lines = [jnp.where(here, bests[q], jnp.bfloat16(0)) for q in snaps]
    slot_of = left(iota((t, 1), 0), plan.slots)
    lanes = [hot((t, LANES), 1, q * plan.slots + slot_of) for q in snaps]
    tail = dot(jnp.concatenate(lines, axis=1), jnp.concatenate(lanes, axis=0), 1, 0).astype(jnp.bfloat16)
    width = plan.width
    if plan.aligned:
        for r in cores:
            for p in range(n):
                base = plan.at(p, r, plan.back)
                for q in snaps:
                    a = base + q * plan.slots
                    out_ref[a : a + plan.slots, :] = blends[q][
                        p * plan.slots : (p + 1) * plan.slots, r * width : (r + 1) * width
                    ]
                out_ref[base + plan.data : base + plan.back, :] = tail[p * SUB : p * SUB + plan.back - plan.data]
        return
    height = n * plan.groups * plan.back
    col = iota((1, n * tall), 1)
    full = None
    for r in cores:
        piece = dot(hot((height, n * tall), 0, plan.at(col // tall, r, tall) + col % tall), tail, 1, 0)
        for q in snaps:
            put = hot((height, t), 0, plan.at(source, r, plan.back) + q * plan.slots + slot)
            piece = piece + dot(put, blends[q][:, r * width : (r + 1) * width], 1, 0)
        full = piece if full is None else full + piece
    out_ref[...] = full.astype(jnp.bfloat16)


def land_kernel(plan, back_ref, target_ref, rows_ref, out_ref, best_ref):
    h, t = plan.halos, plan.total
    target = target_ref[...]
    column = jnp.transpose(target)
    for g in range(plan.groups):
        tail, row = tail_in(plan, back_ref, g, plan.back)
        pulls = []
        for q in range(plan.per):
            s = g * plan.per + q
            spot = column[:, s : s + 1]
            owner, slot = spot >> 7, (spot & (LANES - 1)) - q * plan.slots
            take = hot((h, t), 1, jnp.where(spot >= 0, owner * plan.slots + slot, -1))
            rows = dot(take, rows_in(plan, back_ref, g, q, plan.back), 1, 0)
            rows = jnp.where(jnp.broadcast_to(spot, (h, plan.width)) >= 0, rows, rows_ref[s].astype(jnp.float32))
            out_ref[s] = rows.astype(jnp.bfloat16)
            spot = target[s : s + 1, :]
            pulls.append(hot((tail.shape[0], h), 0, jnp.where(spot >= 0, row(spot >> 7), -1)))
        grid = dot(tail, jnp.concatenate(pulls, axis=1), 0, 0)
        for q in range(plan.per):
            s = g * plan.per + q
            place = target[s : s + 1, :] & (LANES - 1)
            mine = jnp.where(iota((LANES, h), 0) == place, grid[:, q * h : (q + 1) * h], 0.0)
            best_ref[s : s + 1, :] = jnp.sum(mine, axis=0, keepdims=True).astype(jnp.bfloat16)


def body(halo_rows, unmatched, owner_id, cand_index, lengths, choice_index, desc_rows):
    peers, groups = lax.axis_size("space"), lax.axis_size("rep")
    snaps, halos, width = halo_rows.shape
    cands, listed = desc_rows.shape[1], cand_index.shape[2]
    plan = Plan(peers, groups, snaps, halos, width, cands, listed)
    rep = lax.axis_index("rep").astype(jnp.int32)

    def swap(flat, size):
        boxed = flat.reshape(peers * groups, size // 2, 2, width)
        boxed = lax.all_to_all(boxed, ("space", "rep"), 0, 0, tiled=True)
        return boxed.reshape(peers * groups * size, width)

    other = lax.ppermute(desc_rows, "rep", [(0, 1), (1, 0)])

    vmem = pl.BlockSpec(memory_space=pltpu.VMEM)
    smem = pl.BlockSpec(memory_space=pltpu.SMEM)
    hbm = pl.BlockSpec(memory_space=pltpu.HBM)
    small = pltpu.CompilerParams(vmem_limit_bytes=20 << 20)
    packed = pltpu.CompilerParams(vmem_limit_bytes=20 << 20)
    flat = (snaps, halos)
    upper = pl.pallas_call(
        lambda *refs: order_kernel(plan, *refs),
        name="order",
        compiler_params=pltpu.CompilerParams(vmem_limit_bytes=66_600_000),
        cost_estimate=pl.CostEstimate(flops=1 << 32, bytes_accessed=0, transcendentals=0),
        out_shape=pltpu.VMEM((halos, halos), jnp.bfloat16),
        out_specs=vmem,
    )()
    sent, target = pl.pallas_call(
        lambda *refs: route_kernel(plan, *refs),
        name="route",
        compiler_params=small,
        out_shape=(
            jax.ShapeDtypeStruct((peers * groups * plan.send, width), jnp.bfloat16),
            jax.ShapeDtypeStruct(flat, jnp.int32),
        ),
        in_specs=[smem] + [vmem] * 7,
        out_specs=(vmem, vmem),
    )(
        rep.reshape(1),
        upper,
        owner_id.reshape(flat),
        unmatched,
        jnp.swapaxes(cand_index, 1, 2),
        lengths,
        choice_index,
        halo_rows,
    )
    got = swap(sent, plan.send)
    peek = got[0:SUB] * jnp.bfloat16(2)
    reply = pl.pallas_call(
        lambda *refs: owner_kernel(plan, *refs),
        name="owner",
        compiler_params=packed,
        out_shape=jax.ShapeDtypeStruct((peers * groups * plan.back, width), jnp.bfloat16),
        in_specs=[smem, vmem, vmem, vmem, vmem],
        out_specs=vmem,
        scratch_shapes=[
            pltpu.VMEM((plan.per, 2, listed, plan.total), jnp.int32),
            pltpu.VMEM((plan.per, cands // WORD, plan.total), jnp.int32),
        ],
    )(rep.reshape(1), got, desc_rows, other, peek)
    back = swap(reply, plan.back)
    return pl.pallas_call(
        lambda *refs: land_kernel(plan, *refs),
        name="land",
        compiler_params=packed,
        out_shape=(
            jax.ShapeDtypeStruct((snaps, halos, width), jnp.bfloat16),
            jax.ShapeDtypeStruct((snaps, halos), jnp.bfloat16),
        ),
        in_specs=[vmem] * 3,
        out_specs=(vmem, vmem),
    )(back, target, halo_rows)


def solution(mesh):
    in_specs = (
        P(None, "space", "rep"),
        P(None, "space"),
        P(None, "space", None),
        P(None, "space", None),
        P(None, "space"),
        P(None, "space"),
        P(None, "space", "rep"),
    )
    out_specs = (P(None, "space", "rep"), P(None, "space"))

    return jax.shard_map(body, mesh=mesh, in_specs=in_specs, out_specs=out_specs, check_vma=False)
```
